32 devices in a mesh: lon: 4 (over z), lat: 8 (over y, x, core).
Axes of the slice: x: 2, y: 2, z: 4, core: 2. Of those that a mesh axis runs over, the one named last changes fastest.
Arguments:
- travel_times: float32 [1024], P(('lon', 'lat')), may hold values from -6 to 6
- ray_counts: int32 [32], P(('lon', 'lat')), may hold values from 4 to 32
- tile_brick: int32 [1024, 4], P(('lon', 'lat')), may hold values from 0 to 31, all different within a row; in each aligned block of 32 rows (0 to 31, 32 to 63, ...) at most 8 rows name the same one
- cell_offsets: int32 [1024, 4, 128], P(('lon', 'lat')), may hold values from 0 to 1023
- cell_depths: int32 [1024, 4, 128], P(('lon', 'lat')), may hold values from 0 to 127
- seg_lengths: float32 [1024, 4, 128], P(('lon', 'lat')), may hold values from 0.002 to 0.02
Outputs:
- model: float32 [128, 256, 128], P('lon', 'lat')
- misfit: float32 [1024], P(('lon', 'lat'))
The draws below stay inside these ranges and needn't reach their ends.
Inputs may be any that keep to these rules, and one draw needn't show every extreme that they name: `tile_brick`: among the 4 tiles of all rays of one device, no brick is named more than 8 times, a bound that some block reaches; a ray's tiles name different bricks; brick k lives on the device at position k of lon+lat. Only the first ray_counts rays of a device's 32 slots are live.
All inputs are finite; a program needn't handle non-finite values.
Results may differ from the reference program's by a relative error of at most 0.0014.
Values sent between devices are 32-bit elements; how exact they have to be, the bound alone decides.
No kernel may reach another device: no remote copies, remote signals or barrier semaphores. Data moves between devices by JAX's collectives and lax.ppermute only.
A program may use at most 64 MiB of HBM per device.

```python
import math
import jax
import jax.numpy as jnp
import numpy as np
from jax import lax

CLON = 32
CLAT = 32
DEP = 128
SEG = 128
TPR = 4
RAYS_DEV = 32
ITERS = 2
CAP = 8
RAYS = 1024
N_LON = 4
N_LAT = 8
DEVICES = 32


def touch_ends(values, stream_key, smallest, largest):
    longest = values.shape.index(max(values.shape))
    spots = []
    for shift in (0, 1):
        where = [jax.random.randint(jax.random.fold_in(stream_key, axis), (), 0, length) for axis, length in enumerate(values.shape)]
        where[longest] = (where[longest] + shift) % values.shape[longest]
        spots.append(tuple(where))
    return values.at[spots[0]].set(smallest).at[spots[1]].set(largest)


def shard_levels(own_key, extent, pieces, smallest, high):
    def one(axis_at, shards_of):
        steps = jax.random.uniform(jax.random.fold_in(jax.random.fold_in(own_key, 6), axis_at), (shards_of,), jnp.float32, smallest / len(pieces), high / len(pieces))
        return jnp.repeat(jnp.exp(steps), extent[axis_at] // shards_of).reshape((-1,) + (1,) * (len(extent) - axis_at - 1))

    factor_of = one(*pieces[0])
    for cut in pieces[1:]:
        factor_of = factor_of * one(*cut)
    return factor_of


def shared_out(stream_key, own, number, rows, count, top, bound, lean):
    sequence = jax.random.permutation(stream_key, count)
    heavy_load, usual = portions_of(count, rows * top, bound, lean, True), portions_of(count, rows * top, bound, lean, False)
    places = jnp.arange(count)

    def named(lengths, rotation):
        used = int((lengths > 0).sum())
        fixed = max(1, used // 4)
        passed = fixed + (places - fixed + rotation * (used - fixed)) % max(1, count - fixed)
        return jnp.zeros((count,), jnp.int32).at[sequence[jnp.where(places < fixed, places, passed)]].set(jnp.asarray(lengths, jnp.int32))

    lengths = jnp.where(number % 4 == 0, named(heavy_load, number // 4), named(usual, number - number // 4 - 1))
    mixed = jax.random.permutation(jax.random.fold_in(own, 3), count)
    donor, sink = mixed[0:count // 2 * 2:2], mixed[1:count // 2 * 2:2]
    margin = jnp.minimum(lengths[donor] - 1, bound - lengths[sink]) // 2
    margin = jnp.where((donor == sequence[0]) | (sink == sequence[0]) | (lengths[sink] == 0), 0, jnp.maximum(margin, 0))
    passed = jax.random.randint(jax.random.fold_in(own, 4), (count // 2,), 0, 1 << 20) % (margin + 1)
    lengths = lengths.at[donor].add(-passed).at[sink].add(passed)
    labels = jnp.searchsorted(jnp.cumsum(lengths), jnp.arange(rows * top), side="right").astype(jnp.int32)
    listing = labels.reshape(top, rows).T
    listing = listing[jax.random.permutation(jax.random.fold_in(own, 1), rows)]
    rotation = jax.random.randint(jax.random.fold_in(own, 2), (rows, 1), 0, top)
    return jnp.take_along_axis(listing, (jnp.arange(top)[None, :] + rotation) % top, axis=1)


def portions_of(number_of, total, most, lean, full):
    portions = [(1 << 20) // math.isqrt(grade ** lean) + 1 for grade in range(1, number_of + 1)]
    largest = most if full else min(most, max(-(-total // number_of), total * portions[0] // sum(portions)))
    least = 1 if total - largest >= number_of - 1 else 0
    holding, surplus = [largest] + [least] * (number_of - 1), total - largest - least * (number_of - 1)
    while surplus > 0:
        movable = [i for i in range(1, number_of) if holding[i] < largest] or [i for i in range(1, number_of) if holding[i] < most]
        whole, budget = sum([portions[i] for i in movable]), surplus
        for i in movable:
            extra = min(most - holding[i], max(1, budget * portions[i] // whole), surplus)
            holding[i] = holding[i] + extra
            surplus = surplus - extra
    return np.array(holding)


def normal_values(own_key, dims, spread, limit, split=(), held_as=jnp.bfloat16):
    values = spread * jax.random.normal(own_key, dims, jnp.float32)
    if split:
        values = values * shard_levels(own_key, dims, split, -0.22, 0.18)
    return jnp.clip(values, -limit, limit).astype(held_as)


def setup_inputs(seed: int = 0) -> dict:
    keys = jax.random.split(jax.random.key(seed), 7)
    travel_times = normal_values(keys[0], (RAYS,), 1.0, 6.0, ((0, 32),), jnp.float32)
    ray_counts = touch_ends(jax.random.randint(keys[1], (DEVICES,), RAYS_DEV // 8, RAYS_DEV + 1), jax.random.fold_in(keys[1], 1), RAYS_DEV // 8, RAYS_DEV).astype(jnp.int32)
    tile_brick_keys = jax.random.split(jax.random.fold_in(keys[2], 1), RAYS // RAYS_DEV)
    tile_brick_turns = jax.random.permutation(jax.random.fold_in(keys[2], 3), RAYS // RAYS_DEV)
    tile_brick = jax.vmap(lambda own, number: shared_out(jax.random.fold_in(keys[2], 2), own, number, RAYS_DEV, DEVICES, TPR, CAP, 2))(tile_brick_keys, tile_brick_turns).reshape((RAYS, TPR))
    cell_offsets = touch_ends(jax.random.randint(keys[3], (RAYS, TPR, SEG), 0, CLON * CLAT), jax.random.fold_in(keys[3], 1), 0, (CLON * CLAT) - 1).astype(jnp.int32)
    cell_depths = touch_ends(jax.random.randint(keys[4], (RAYS, TPR, SEG), 0, DEP), jax.random.fold_in(keys[4], 1), 0, DEP - 1).astype(jnp.int32)
    seg_lengths = jnp.clip(0.002 + 0.018 * jax.random.uniform(keys[5], (RAYS, TPR, SEG), jnp.float32) ** shard_levels(keys[5], (RAYS, TPR, SEG), ((0, 32),), -0.2, 0.2), 0.002, 0.02)
    return {"travel_times": travel_times, "ray_counts": ray_counts, "tile_brick": tile_brick, "cell_offsets": cell_offsets, "cell_depths": cell_depths, "seg_lengths": seg_lengths}


damping = 0.01

def to_bricks(grid):
    parts = grid.reshape(N_LON, CLON, N_LAT, CLAT, DEP).transpose(0, 2, 1, 3, 4)
    return parts.reshape(N_LON * N_LAT * CLON * CLAT * DEP)

def from_bricks(flat_cells):
    parts = flat_cells.reshape(N_LON, N_LAT, CLON, CLAT, DEP).transpose(0, 2, 1, 3, 4)
    return parts.reshape(N_LON * CLON, N_LAT * CLAT, DEP)

def smoothing(field):
    lon_pad = jnp.concatenate([field[-1:], field, field[:1]], axis=0)
    lat_pad = jnp.pad(field, ((0, 0), (1, 1), (0, 0)))
    dep_pad = jnp.pad(field, ((0, 0), (0, 0), (1, 1)))
    result = 6.0 * field - lon_pad[2:] - lon_pad[:-2] - lat_pad[:, 2:] - lat_pad[:, :-2]
    return result - dep_pad[:, :, 2:] - dep_pad[:, :, :-2]

def reference(travel_times, ray_counts, tile_brick, cell_offsets, cell_depths, seg_lengths):
    rays_all = travel_times.shape[0]
    ray_pos = jnp.arange(rays_all, dtype=jnp.int32)
    owner_dev = ray_pos // RAYS_DEV
    live_mask = (ray_pos % RAYS_DEV < ray_counts[owner_dev]).astype(jnp.float32)
    weights = (seg_lengths * live_mask[:, None, None]).reshape(-1)
    brick_cells = CLON * CLAT * DEP
    inside = cell_offsets * DEP + cell_depths
    cell_index = (tile_brick[:, :, None] * brick_cells + inside).astype(jnp.int32).reshape(-1)
    total_cells = N_LON * N_LAT * brick_cells

    def forward(grid):
        cells = to_bricks(grid)
        return lax.optimization_barrier(jnp.sum((weights * cells[cell_index]).reshape(rays_all, -1), axis=1))

    def backward(ray_vals):
        terms = (weights.reshape(rays_all, -1) * ray_vals[:, None]).reshape(-1)
        cells = jnp.zeros((total_cells,), jnp.float32).at[cell_index].add(terms)
        return from_bricks(cells)
    data = travel_times * live_mask
    beta_now = jnp.sqrt(jnp.sum(data * data))
    u_ray = data / beta_now
    u_grid = jnp.zeros((N_LON * CLON, N_LAT * CLAT, DEP), jnp.float32)
    v_dir = backward(u_ray)
    alpha_now = jnp.sqrt(jnp.sum(v_dir * v_dir))
    v_dir = v_dir / alpha_now
    search = v_dir
    model = jnp.zeros_like(v_dir)
    phi_bar = beta_now
    rho_bar = alpha_now
    for turn_index in range(ITERS):
        u_ray = forward(v_dir) - alpha_now * u_ray
        u_grid = damping * smoothing(v_dir) - alpha_now * u_grid
        beta_now = jnp.sqrt(jnp.sum(u_ray * u_ray) + jnp.sum(u_grid * u_grid))
        u_ray = u_ray / beta_now
        u_grid = u_grid / beta_now
        v_dir = backward(u_ray) + damping * smoothing(u_grid) - beta_now * v_dir
        alpha_now = jnp.sqrt(jnp.sum(v_dir * v_dir))
        v_dir = v_dir / alpha_now
        rho_new = jnp.sqrt(rho_bar * rho_bar + beta_now * beta_now)
        cosine = rho_bar / rho_new
        sine_val = beta_now / rho_new
        theta_val = sine_val * alpha_now
        rho_bar = -cosine * alpha_now
        phi_val = cosine * phi_bar
        phi_bar = sine_val * phi_bar
        model = model + phi_val / rho_new * search
        search = v_dir - theta_val / rho_new * search
    misfit = data - forward(model)
    return (model, misfit)
```

```python
import jax
import jax.numpy as jnp
from jax import lax
from jax.experimental import pallas as pl
from jax.experimental.pallas import tpu as pltpu
from jax.sharding import PartitionSpec as P

CLON = 32
CLAT = 32
DEP = 128
COLS = CLON * CLAT
ROWS_M = COLS // 2
ROWS_N = 2 * DEP
CH = 8

damping = 0.01
AXES = ("lon", "lat")
f32 = jnp.float32
i32 = jnp.int32
bf16 = jnp.bfloat16
SM = pl.BlockSpec(memory_space=pltpu.SMEM)
VM = pl.BlockSpec(memory_space=pltpu.VMEM)


def iota(shape, dim):
    return lax.broadcasted_iota(i32, shape, dim)


def sds(shape, dtype=f32):
    return jax.ShapeDtypeStruct(shape, dtype)


def call(kernel, outs, ins, args, scratch=(), out_specs=None, name=None):
    return pl.pallas_call(
        kernel,
        out_shape=outs,
        in_specs=list(ins),
        out_specs=out_specs if out_specs is not None else [VM] * len(outs),
        scratch_shapes=list(scratch),
        name=name,
    )(*args)


def pack_kernel(devices, cap, rays, per_ray):
    width = 2 * cap + 1

    def kernel(brick, counts, times, offs, deps, lens, out, cells, used):
        lane = iota((1, 128), 1)
        out[...] = jnp.zeros_like(out)
        o = offs[...]
        cells[...] = ((o & (ROWS_M - 1)) * ROWS_N + (o >> 9) * DEP + deps[...]).astype(f32)

        def clear(d, carry):
            used[d] = 0
            return carry

        lax.fori_loop(0, devices, clear, 0)

        def one(r, row):
            value = times[r]
            for j in range(per_ray):
                b = brick[r, j]
                k = used[b]
                used[b] = k + 1
                base = b * width
                out[base + k] = cells[pl.ds(r * per_ray + j, 1), :]
                out[base + cap + k] = lens[pl.ds(r * per_ray + j, 1), :]
                extra = out[base + 2 * cap]
                extra = jnp.where(lane == k, r.astype(f32), extra)
                out[base + 2 * cap] = jnp.where(lane == 16 + k, value, extra)
            return jnp.where(lane == 64 + r, value, row)

        row = lax.fori_loop(0, counts[0], one, jnp.zeros((1, 128), f32))

        def finish(d, carry):
            at = d * width + 2 * cap
            extra = jnp.where(lane >= 64, row, out[at])
            out[at] = jnp.where(lane == 127, used[d].astype(f32), extra)
            return carry

        lax.fori_loop(0, devices, finish, 0)

    return kernel


def split(x):
    high = x.astype(bf16).astype(f32)
    return high, x - high


def lanes_of(block, i, n):
    return jnp.concatenate([block[i + j : i + j + 1, :] for j in range(n)], axis=1)


GROUP = 4


def scatter_tiles(total, cell_ref, w_ref, b_ref, acc):
    acc[...] = jnp.zeros_like(acc)
    seg = GROUP * 128
    im = iota((ROWS_M, seg), 0)
    inn = iota((ROWS_N, seg), 0)
    zero = jnp.zeros((), f32)

    def chunk(c, carry):
        at = pl.multiple_of(c * CH, CH)
        ci = cell_ref[pl.ds(at, CH), :].astype(i32)
        m = ci >> 8
        n = ci & (ROWS_N - 1)
        high, low = split(w_ref[pl.ds(at, CH), :] * b_ref[pl.ds(at, CH), :])
        for i in range(0, CH, GROUP):
            ohm = jnp.where(im == lanes_of(m, i, GROUP), 1.0, 0.0).astype(bf16)
            hit = inn == lanes_of(n, i, GROUP)
            vh = jnp.where(hit, lanes_of(high, i, GROUP), zero).astype(bf16)
            vl = jnp.where(hit, lanes_of(low, i, GROUP), zero).astype(bf16)
            dims = (((1,), (1,)), ((), ()))
            acc[...] += lax.dot_general(
                ohm, vh, dims, preferred_element_type=f32
            ) + lax.dot_general(ohm, vl, dims, preferred_element_type=f32)
        return carry

    lax.fori_loop(0, (total + CH - 1) // CH, chunk, 0)


def gather_tiles(total, cell_ref, w_ref, gh, gl, yv):
    yv[...] = jnp.zeros_like(yv)
    seg = 256
    im = iota((ROWS_M, seg), 0)
    inn = iota((ROWS_N, seg), 0)

    def chunk(c, carry):
        at = pl.multiple_of(c * CH, CH)
        ci = cell_ref[pl.ds(at, CH), :].astype(i32)
        m = ci >> 8
        n = ci & (ROWS_N - 1)
        rows = []
        for i in range(0, CH, 2):
            ohn = jnp.where(inn == lanes_of(n, i, 2), 1.0, 0.0).astype(bf16)
            full = jnp.dot(gh[...], ohn, preferred_element_type=f32) + jnp.dot(
                gl[...], ohn, preferred_element_type=f32
            )
            got = jnp.sum(jnp.where(im == lanes_of(m, i, 2), full, 0.0), axis=0, keepdims=True)
            rows += [got[:, :128], got[:, 128:]]
        yv[pl.ds(at, CH), :] = jnp.concatenate(rows, axis=0) * w_ref[pl.ds(at, CH), :]
        return carry

    lax.fori_loop(0, (total + CH - 1) // CH, chunk, 0)


def layers(src, lo, hi, la, lb):
    lo[...] = src[0:CLAT, :]
    hi[...] = src[COLS - CLAT : COLS, :]
    for i in range(CLON):
        la[i] = src[i * CLAT : i * CLAT + 1, :]
        lb[i] = src[(i + 1) * CLAT - 1 : (i + 1) * CLAT, :]


LAYERS = [(CLAT, DEP), (CLAT, DEP), (CLON, 1, DEP), (CLON, 1, DEP)]


def stencil_layer(i, src, before, after, lat_before, lat_after):
    sub = iota((CLAT, DEP), 0)
    lane = iota((CLAT, DEP), 1)
    c = src[i * CLAT : (i + 1) * CLAT, :]
    up = before[...] if i == 0 else src[(i - 1) * CLAT : i * CLAT, :]
    down = after[...] if i == CLON - 1 else src[(i + 1) * CLAT : (i + 2) * CLAT, :]
    lm = jnp.where(sub == 0, lat_before[i], pltpu.roll(c, 1, 0))
    lp = jnp.where(sub == CLAT - 1, lat_after[i], pltpu.roll(c, CLAT - 1, 0))
    dm = jnp.where(lane == 0, 0.0, pltpu.roll(c, 1, 1))
    dp = jnp.where(lane == DEP - 1, 0.0, pltpu.roll(c, DEP - 1, 1))
    return 6.0 * c - up - down - lm - lp - dm - dp


def colsum(x):
    return jnp.sum(x, axis=0, keepdims=True)


def start_kernel(devices, cap, rays):
    width = 2 * cap + 1

    def kernel(cnt, recv, g, lo, hi, la, lb, cell, w, q, data, total, b, acc):
        sub = iota((cap, 128), 0)
        lane = iota((cap, 128), 1)
        lane1 = iota((1, 128), 1)
        q[...] = jnp.full_like(q, -1.0)
        per_row = 128 // rays
        pos = 0
        row = jnp.zeros((1, 128), f32)
        for s in range(devices):
            at = s * width
            ext = recv[at + 2 * cap]
            wide = jnp.broadcast_to(ext, (cap, 128))
            qs = jnp.sum(jnp.where(lane == sub, wide, 0.0), axis=1, keepdims=True)
            bs = jnp.sum(jnp.where(lane == sub + 16, wide, 0.0), axis=1, keepdims=True)
            cell[pl.ds(pos, cap), :] = jnp.concatenate([recv[at + k] for k in range(cap)], axis=0)
            w[pl.ds(pos, cap), :] = jnp.concatenate(
                [recv[at + cap + k] for k in range(cap)], axis=0
            )
            q[pl.ds(pos, cap), :] = jnp.broadcast_to(qs + float(s * rays), (cap, 128))
            b[pl.ds(pos, cap), :] = jnp.broadcast_to(bs, (cap, 128))
            pos = pos + cnt[s]
            j = s % per_row
            moved = pltpu.roll(ext, (j * rays - 64) % 128, 1)
            inside = (lane1 >= j * rays) & (lane1 < (j + 1) * rays)
            row = jnp.where(inside, moved, row)
            if j == per_row - 1:
                data[s // per_row : s // per_row + 1, :] = row
        w[pl.ds(pos, CH), :] = jnp.zeros((CH, 128), f32)
        b[pl.ds(pos, CH), :] = jnp.zeros((CH, 128), f32)
        q[pl.ds(pos, CH), :] = jnp.full((CH, 128), -1.0, f32)
        total[0] = pos
        scatter_tiles(pos, cell, w, b, acc)
        g[0:ROWS_M, :] = acc[:, :DEP]
        g[ROWS_M:COLS, :] = acc[:, DEP:]
        layers(g, lo, hi, la, lb)

    return kernel


def ray_onehots(q):
    qi = q[...].astype(i32)
    lane = iota(qi.shape, 1)
    return jnp.where((qi >> 7) == lane, 1.0, 0.0), (qi & 127) == lane


def forward_kernel(ray_rows):
    def kernel(total, src, cell, w, q, y, gh, gl, yv):
        for half in range(2):
            rows = slice(half * ROWS_M, (half + 1) * ROWS_M)
            cols = slice(half * DEP, (half + 1) * DEP)
            high, low = split(src[rows, :])
            gh[:, cols] = high.astype(bf16)
            gl[:, cols] = low.astype(bf16)
        gather_tiles(total[0], cell, w, gh, gl, yv)
        oh, ql = ray_onehots(q)
        ys = jnp.where(ql, jnp.sum(yv[...], axis=1, keepdims=True), 0.0)
        full = lax.dot_general(
            oh,
            ys,
            (((0,), (0,)), ((), ())),
            precision=lax.Precision.HIGHEST,
            preferred_element_type=f32,
        )
        y[...] = full[:ray_rows, :]

    return kernel


def send_copies(out, devices, rows):
    count = len(rows)

    def one(d, carry):
        for i, row in enumerate(rows):
            out[d * count + i] = row
        return carry

    lax.fori_loop(0, devices, one, 0)


def smooth_kernel(devices, ray_rows):
    def kernel(g, before, after, lat_before, lat_after, y, q1, lo, hi, la, lb, out):
        gg = jnp.zeros((CLAT, DEP), f32)
        qq = jnp.zeros((CLAT, DEP), f32)
        for i in range(CLON):
            res = stencil_layer(i, g, before, after, lat_before, lat_after)
            q1[i * CLAT : (i + 1) * CLAT, :] = res
            c = g[i * CLAT : (i + 1) * CLAT, :]
            gg = gg + c * c
            qq = qq + res * res
        layers(q1, lo, hi, la, lb)
        rows = [y[i : i + 1, :] for i in range(ray_rows)] + [colsum(gg), colsum(qq)]
        send_copies(out, devices, rows)

    return kernel


def received(recv, devices, count):
    def one(d, acc):
        return acc + recv[pl.ds(d * count, count)]

    return lax.fori_loop(0, devices, one, jnp.zeros((count, 1, 128), f32))


def all_rows(acc, start, count):
    return jnp.concatenate([acc[start + i] for i in range(count)], axis=0)


def total_of(x):
    return jnp.sum(jnp.sum(x, axis=0, keepdims=True), axis=1, keepdims=True)


def first_scalars(recv, data, devices, ray_rows):
    acc = received(recv, devices, ray_rows + 2)
    p1 = all_rows(acc, 0, ray_rows)
    gg = total_of(acc[ray_rows])
    qq = total_of(acc[ray_rows + 1])
    beta1 = jnp.sqrt(total_of(data * data))
    nrm = jnp.sqrt(gg)
    alpha1 = nrm / beta1
    av1 = p1 / nrm
    r2 = av1 - alpha1 * (data / beta1)
    beta2 = jnp.sqrt(total_of(r2 * r2) + (damping * damping) * (qq / gg))
    return av1, r2 / beta2, nrm, beta1, alpha1, beta2, qq


def second_kernel(devices, ray_rows):
    def kernel(
        total, recv, data, g, q1, before, after, lat_before, lat_after, cell, w, q,
        v, lo, hi, la, lb, av, u2, num, b, acc,
    ):
        av1, u, nrm, beta1, alpha1, beta2, qq = first_scalars(recv, data[...], devices, ray_rows)
        av[...] = av1
        u2[...] = u
        numbers = [nrm, beta1, alpha1, beta2, qq]
        lane = iota((1, 128), 1)
        packed = jnp.zeros((1, 128), f32)
        for i, x in enumerate(numbers):
            packed = jnp.where(lane == i, x, packed)
        num[...] = packed
        oh, ql = ray_onehots(q)
        padded = jnp.concatenate([u, jnp.zeros((128 - ray_rows, 128), f32)], axis=0)
        picked = jnp.dot(oh, padded, precision=lax.Precision.HIGHEST, preferred_element_type=f32)
        picked = jnp.sum(jnp.where(ql, picked, 0.0), axis=1, keepdims=True)
        b[...] = jnp.broadcast_to(picked, b.shape)
        scatter_tiles(total[0], cell, w, b, acc)
        a = (damping * damping) / (nrm * beta2)
        e = beta2 / nrm
        for i in range(CLON):
            half, at = divmod(i * CLAT, ROWS_M)
            h = acc[at : at + CLAT, half * DEP : (half + 1) * DEP]
            res = stencil_layer(i, q1, before, after, lat_before, lat_after)
            v[i * CLAT : (i + 1) * CLAT, :] = h + a * res - e * g[i * CLAT : (i + 1) * CLAT, :]
        layers(v, lo, hi, la, lb)

    return kernel


def last_smooth_kernel(devices, ray_rows):
    def kernel(v, q1, before, after, lat_before, lat_after, y, out):
        vv = jnp.zeros((CLAT, DEP), f32)
        ll = jnp.zeros((CLAT, DEP), f32)
        lq = jnp.zeros((CLAT, DEP), f32)
        for i in range(CLON):
            res = stencil_layer(i, v, before, after, lat_before, lat_after)
            c = v[i * CLAT : (i + 1) * CLAT, :]
            vv = vv + c * c
            ll = ll + res * res
            lq = lq + res * q1[i * CLAT : (i + 1) * CLAT, :]
        rows = [y[i : i + 1, :] for i in range(ray_rows)] + [colsum(vv), colsum(ll), colsum(lq)]
        send_copies(out, devices, rows)

    return kernel


def final_kernel(devices, ray_rows, rays):
    def kernel(me, recv, data, av, u2, num, g, v, model, misfit):
        acc = received(recv, devices, ray_rows + 3)
        p2 = all_rows(acc, 0, ray_rows)
        vv = total_of(acc[ray_rows])
        ll = total_of(acc[ray_rows + 1])
        lq = total_of(acc[ray_rows + 2])
        nrm, beta1, alpha1, beta2, qq = [num[0:1, i : i + 1] for i in range(5)]
        alpha2 = jnp.sqrt(vv)
        av2 = p2 / alpha2
        r3 = av2 - alpha2 * u2[...]
        x = alpha2 / (nrm * beta2)
        grid = ll / vv - 2.0 * (x / alpha2) * lq + (x * x) * qq
        beta3sq = total_of(r3 * r3) + (damping * damping) * grid
        rho = jnp.sqrt(alpha1 * alpha1 + beta2 * beta2)
        cosine = alpha1 / rho
        sine = beta2 / rho
        theta = sine * alpha2
        rho_bar = -cosine * alpha2
        k1 = cosine * beta1 / rho
        t = theta / rho
        phi_bar = sine * beta1
        rho2 = jnp.sqrt(rho_bar * rho_bar + beta3sq)
        k2 = (rho_bar / rho2) * phi_bar / rho2
        first = k1 - k2 * t
        model[...] = (first / nrm) * g[...] + (k2 / alpha2) * v[...]
        mis = data[...] - (first * av[...] + k2 * av2)
        per_row = 128 // rays
        d = me[0]
        sub = iota(mis.shape, 0)
        mine = colsum(jnp.where(sub == d // per_row, mis, 0.0))
        misfit[...] = pltpu.roll(mine, (128 - (d % per_row) * rays) % 128, 1)

    return kernel


def exchange_all(x):
    return lax.all_to_all(x, AXES, split_axis=0, concat_axis=0, tiled=True)


def halo(parts):
    lo, hi, la, lb = parts

    def ring(axis, wrap):
        n = lax.axis_size(axis)
        up = [(i, (i + 1) % n) for i in range(n if wrap else n - 1)]
        return up, [(j, i) for i, j in up]

    up, down = ring("lon", True)
    lat_up, lat_down = ring("lat", False)
    return (
        lax.ppermute(hi, "lon", up),
        lax.ppermute(lo, "lon", down),
        lax.ppermute(lb, "lat", lat_up),
        lax.ppermute(la, "lat", lat_down),
    )


def shards(travel_times, ray_counts, tile_brick, cell_offsets, cell_depths, seg_lengths):
    devices = lax.axis_size(AXES)
    rays, per_ray, segs = cell_offsets.shape
    tiles = rays * per_ray
    slots = 2 * tiles
    cap = slots // devices
    width = 2 * cap + 1
    ray_rows = devices * rays // 128
    room = slots + CH
    flat = lambda x: x.reshape(tiles, segs)
    layer_outs = [sds(s) for s in LAYERS]
    grid = sds((COLS, DEP))
    buf = lambda dtype: pltpu.VMEM((ROWS_M, ROWS_N), dtype)

    (packed,) = call(
        pack_kernel(devices, cap, rays, per_ray),
        [sds((devices * width, 1, 128))],
        [SM, SM, SM, VM, VM, VM],
        (tile_brick, ray_counts, travel_times, flat(cell_offsets), flat(cell_depths), flat(seg_lengths)),
        [pltpu.VMEM((tiles, segs), f32), pltpu.SMEM((devices,), i32)],
        name="pack",
    )
    recv0 = exchange_all(packed)
    counts = recv0.reshape(devices, width, 128)[:, 2 * cap, 127].astype(i32)
    g, *edges, cell, w, q, data, total = call(
        start_kernel(devices, cap, rays),
        [grid, *layer_outs, sds((room, 128)), sds((room, 128)), sds((room, 128)), sds((ray_rows, 128)), sds((1,), i32)],
        [SM, VM],
        (counts, recv0),
        [pltpu.VMEM((room, 128), f32), buf(f32)],
        out_specs=[VM] * 9 + [SM],
        name="start",
    )
    gather_scratch = [buf(bf16), buf(bf16), pltpu.VMEM((room, 128), f32)]
    around = halo(edges)
    (y1,) = call(
        forward_kernel(ray_rows), [sds((ray_rows, 128))], [SM] + [VM] * 4, (total, g, cell, w, q),
        gather_scratch, name="forward",
    )
    q1, *edges, send = call(
        smooth_kernel(devices, ray_rows),
        [grid, *layer_outs, sds((devices * (ray_rows + 2), 1, 128))],
        [VM] * 6,
        (g, *around, y1),
        name="smooth",
    )
    around = halo(edges)
    recv1 = exchange_all(send)
    v, *edges, av, u2, num = call(
        second_kernel(devices, ray_rows),
        [grid, *layer_outs, sds((ray_rows, 128)), sds((ray_rows, 128)), sds((1, 128))],
        [SM] + [VM] * 11,
        (total, recv1, data, g, q1, *around, cell, w, q),
        [pltpu.VMEM((room, 128), f32), buf(f32)],
        name="second",
    )
    around = halo(edges)
    (y2,) = call(
        forward_kernel(ray_rows), [sds((ray_rows, 128))], [SM] + [VM] * 4, (total, v, cell, w, q),
        gather_scratch, name="forward",
    )
    (send,) = call(
        last_smooth_kernel(devices, ray_rows),
        [sds((devices * (ray_rows + 3), 1, 128))],
        [VM] * 7,
        (v, q1, *around, y2),
        name="last_smooth",
    )
    recv2 = exchange_all(send)
    me = lax.axis_index(AXES).astype(i32).reshape(1)
    model, mis = call(
        final_kernel(devices, ray_rows, rays),
        [grid, sds((1, 128))],
        [SM] + [VM] * 7,
        (me, recv2, data, av, u2, num, g, v),
        name="final",
    )
    return model.reshape(CLON, CLAT, DEP), mis[0, :rays]


def solution(mesh):
    placed = (
        P(("lon", "lat")),
        P(("lon", "lat")),
        P(("lon", "lat"), None),
        P(("lon", "lat"), None, None),
        P(("lon", "lat"), None, None),
        P(("lon", "lat"), None, None),
    )
    return jax.shard_map(
        shards,
        mesh=mesh,
        in_specs=placed,
        out_specs=(P("lon", "lat", None), P(("lon", "lat"))),
        check_vma=False,
    )
```

```python
import jax
import jax.numpy as jnp
from jax import lax
from jax.experimental import pallas as pl
from jax.experimental.pallas import tpu as pltpu
from jax.sharding import PartitionSpec as P

CLON = 32
CLAT = 32
DEP = 128
COLS = CLON * CLAT
ROWS_M = COLS // 2
ROWS_N = 2 * DEP
CH = 16
BLOCK = 16
WIN = 192

damping = 0.01
AXES = ("lon", "lat")
f32 = jnp.float32
i32 = jnp.int32
bf16 = jnp.bfloat16
SM = pl.BlockSpec(memory_space=pltpu.SMEM)
VM = pl.BlockSpec(memory_space=pltpu.VMEM)


def iota(shape, dim):
    return lax.broadcasted_iota(i32, shape, dim)


def sds(shape, dtype=f32):
    return jax.ShapeDtypeStruct(shape, dtype)


def call(kernel, outs, ins, args, scratch=(), out_specs=None, name=None):
    return pl.pallas_call(
        kernel,
        out_shape=outs,
        in_specs=list(ins),
        out_specs=out_specs if out_specs is not None else [VM] * len(outs),
        scratch_shapes=list(scratch),
        name=name,
    )(*args)


def sort_lanes(key, value):
    lane = iota(key.shape, 1)
    size = 2
    while size <= 128:
        step = size // 2
        while step:
            low = (lane & step) == 0
            other = jnp.where(low, pltpu.roll(key, 128 - step, 1), pltpu.roll(key, step, 1))
            other_value = jnp.where(low, pltpu.roll(value, 128 - step, 1), pltpu.roll(value, step, 1))
            keep_low = low == ((lane & size) == 0)
            swap = (keep_low & (other < key)) | (~keep_low & (other > key))
            key = jnp.where(swap, other, key)
            value = jnp.where(swap, other_value, value)
            step //= 2
        size *= 2
    return key, value


def pack_kernel(devices, cap, rays, per_ray):
    width = 2 * cap + 1

    def kernel(brick, counts, times, offs, deps, lens, out, cells, lengths, used):
        lane = iota((1, 128), 1)
        out[...] = jnp.zeros_like(out)
        o = offs[...]
        key, length = sort_lanes((o & (ROWS_M - 1)) * ROWS_N + (o >> 9) * DEP + deps[...], lens[...])
        cells[...] = key.astype(f32)
        lengths[...] = length

        def clear(d, carry):
            used[d] = 0
            return carry

        lax.fori_loop(0, devices, clear, 0)

        def one(r, row):
            value = times[r]
            for j in range(per_ray):
                b = brick[j, r]
                k = used[b]
                used[b] = k + 1
                base = b * width
                out[base + k] = cells[pl.ds(r * per_ray + j, 1), :]
                out[base + cap + k] = lengths[pl.ds(r * per_ray + j, 1), :]
                extra = out[base + 2 * cap]
                extra = jnp.where(lane == k, r.astype(f32), extra)
                out[base + 2 * cap] = jnp.where(lane == 16 + k, value, extra)
            return jnp.where(lane == 64 + r, value, row)

        row = lax.fori_loop(0, counts[0], one, jnp.zeros((1, 128), f32))

        def finish(d, carry):
            at = d * width + 2 * cap
            extra = jnp.where(lane >= 64, row, out[at])
            out[at] = jnp.where(lane == 127, used[d].astype(f32), extra)
            return carry

        lax.fori_loop(0, devices, finish, 0)

    return kernel


def split(x):
    high = x.astype(bf16).astype(f32)
    return high, x - high


def own_block():
    return (iota((8, 128), 1) >> (BLOCK.bit_length() - 1)) == iota((8, 128), 0)


def side_by_side(rows):
    mine = own_block()
    return jnp.concatenate(
        [colsum(jnp.where(mine, rows[8 * h : 8 * h + 8, :], 0.0)) for h in range(CH // 8)], axis=1
    )


GROUPS = 128 // BLOCK
LANES = CH * BLOCK


def group_tiles(total, cell, w, gcell, gw, base, more):
    def chunk(c, carry):
        at = pl.multiple_of(c * CH, CH)
        turn = lambda ref: jnp.concatenate(
            [
                pltpu.roll(ref[pl.ds(at + 8 * h, 8), :], 0, 1, stride=BLOCK, stride_axis=0)
                for h in range(CH // 8)
            ],
            axis=0,
        )
        cells = turn(cell)
        lens = turn(w)
        rest = jnp.int32(0)
        for j in range(GROUPS):
            gc = side_by_side(pltpu.roll(cells, (128 - j * BLOCK) % 128, 1) if j else cells)
            gl = side_by_side(pltpu.roll(lens, (128 - j * BLOCK) % 128, 1) if j else lens)
            gcell[pl.ds(c * GROUPS + j, 1), :] = gc
            gw[pl.ds(c * GROUPS + j, 1), :] = gl
            m = gc.astype(i32) >> 8
            low = jnp.min(jnp.where(gl != 0.0, m, ROWS_M - 1))
            high = jnp.max(jnp.where(gl != 0.0, m, 0))
            first = jnp.minimum((low >> 4) << 4, ROWS_M - WIN)
            base[c * GROUPS + j] = first
            rest = jnp.maximum(rest, high - first)
        more[c] = (rest + WIN) // WIN
        return carry

    lax.fori_loop(0, (total + CH - 1) // CH, chunk, 0)


def window(first, k, m):
    start = first + k * WIN
    at = pl.multiple_of(jnp.minimum(start, ROWS_M - WIN), 16)
    return at, jnp.where(m >= start, m - at, -1)


def scatter_tiles(total, gcell, gw, base, more, b_ref, acc):
    acc[...] = jnp.zeros_like(acc)
    im = iota((WIN, LANES), 0)
    inn = iota((ROWS_N, LANES), 0)
    dims = (((1,), (1,)), ((), ()))

    def group(g, k, b):
        ci = gcell[pl.ds(g, 1), :].astype(i32)
        at, m = window(base[g], k, ci >> 8)
        n = ci & (ROWS_N - 1)
        high, low = split(gw[pl.ds(g, 1), :] * b)
        ohm = jnp.where(im == m, 1.0, 0.0).astype(bf16)
        hit = inn == n
        vh = jnp.where(hit, high, 0.0).astype(bf16)
        vl = jnp.where(hit, low, 0.0).astype(bf16)
        acc[pl.ds(at, WIN), :] += lax.dot_general(
            ohm, vh, dims, preferred_element_type=f32
        ) + lax.dot_general(ohm, vl, dims, preferred_element_type=f32)

    def chunk(c, carry):
        at = pl.multiple_of(c * CH, CH)
        b = side_by_side(b_ref[pl.ds(at, CH), :])
        for j in range(GROUPS):
            group(c * GROUPS + j, 0, b)

        @pl.when(more[c] > 1)
        def _():
            def again(i, carry):
                group(c * GROUPS + i % GROUPS, 1 + i // GROUPS, b)
                return carry

            lax.fori_loop(0, (more[c] - 1) * GROUPS, again, 0)

        return carry

    lax.fori_loop(0, (total + CH - 1) // CH, chunk, 0)


def gather_tiles(total, gcell, gw, base, more, gh, gl, got, yv):
    yv[...] = jnp.zeros_like(yv)
    im = iota((WIN, LANES), 0)
    inn = iota((ROWS_N, LANES), 0)

    def group(g, k):
        ci = gcell[pl.ds(g, 1), :].astype(i32)
        at, m = window(base[g], k, ci >> 8)
        ohn = jnp.where(inn == (ci & (ROWS_N - 1)), 1.0, 0.0).astype(bf16)
        full = jnp.dot(gh[pl.ds(at, WIN), :], ohn, preferred_element_type=f32) + jnp.dot(
            gl[pl.ds(at, WIN), :], ohn, preferred_element_type=f32
        )
        return colsum(jnp.where(im == m, full, 0.0)) * gw[pl.ds(g, 1), :]

    def chunk(c, carry):
        part = group(c * GROUPS, 0)
        for j in range(1, GROUPS):
            part = part + group(c * GROUPS + j, 0)
        got[...] = part

        @pl.when(more[c] > 1)
        def _():
            def again(i, carry):
                got[...] += group(c * GROUPS + i % GROUPS, 1 + i // GROUPS)
                return carry

            lax.fori_loop(0, (more[c] - 1) * GROUPS, again, 0)

        mine = own_block()
        for h in range(CH // 8):
            at = pl.multiple_of(c * CH + 8 * h, 8)
            yv[pl.ds(at, 8), :] = jnp.where(mine, got[:, 128 * h : 128 * (h + 1)], 0.0)
        return carry

    lax.fori_loop(0, (total + CH - 1) // CH, chunk, 0)


def lat_rows(src, at):
    return src[pl.ds(at, CLON, stride=CLAT), :]


def layers(src, lo, hi, la, lb):
    lo[...] = src[0:CLAT, :]
    hi[...] = src[COLS - CLAT : COLS, :]
    la[...] = lat_rows(src, 0)
    lb[...] = lat_rows(src, CLAT - 1)


LAYERS = [(CLAT, DEP), (CLAT, DEP), (CLON, DEP), (CLON, DEP)]


def depth_part(c):
    lane = iota(c.shape, 1)
    dm = jnp.where(lane == 0, 0.0, pltpu.roll(c, 1, 1))
    dp = jnp.where(lane == DEP - 1, 0.0, pltpu.roll(c, DEP - 1, 1))
    return 6.0 * c - dm - dp


def stencil_rows(c, up, down, lat_before, lat_after):
    sub = iota(c.shape, 0)
    lm = jnp.where(sub == 0, lat_before, pltpu.roll(c, 1, 0))
    lp = jnp.where(sub == CLAT - 1, lat_after, pltpu.roll(c, CLAT - 1, 0))
    return depth_part(c) - up - down - lm - lp


def stencil_layer(i, src, before, after, lat_before, lat_after):
    c = src[i * CLAT : (i + 1) * CLAT, :]
    up = before[...] if i == 0 else src[(i - 1) * CLAT : i * CLAT, :]
    down = after[...] if i == CLON - 1 else src[(i + 1) * CLAT : (i + 2) * CLAT, :]
    return stencil_rows(c, up, down, lat_before[i : i + 1, :], lat_after[i : i + 1, :])


def colsum(x):
    return jnp.sum(x, axis=0, keepdims=True)


def start_kernel(devices, cap, rays):
    width = 2 * cap + 1

    def kernel(
        recv, g, lo, hi, gcell, gw, q, data, total, base, more, cell, w, b, acc
    ):
        sub = iota((cap, 128), 0)
        lane = iota((cap, 128), 1)
        lane1 = iota((1, 128), 1)
        q[...] = jnp.full_like(q, -1.0)
        per_row = 128 // rays
        pos = 0
        row = jnp.zeros((1, 128), f32)
        for s in range(devices):
            at = s * width
            ext = recv[at + 2 * cap]
            wide = jnp.broadcast_to(ext, (cap, 128))
            qs = jnp.sum(jnp.where(lane == sub, wide, 0.0), axis=1, keepdims=True)
            bs = jnp.sum(jnp.where(lane == sub + 16, wide, 0.0), axis=1, keepdims=True)
            cell[pl.ds(pos, cap), :] = jnp.concatenate([recv[at + k] for k in range(cap)], axis=0)
            w[pl.ds(pos, cap), :] = jnp.concatenate(
                [recv[at + cap + k] for k in range(cap)], axis=0
            )
            q[pl.ds(pos, cap), :] = jnp.broadcast_to(qs + float(s * rays), (cap, 128))
            b[pl.ds(pos, cap), :] = jnp.broadcast_to(bs, (cap, 128))
            pos = pos + jnp.max(jnp.where(lane1 == 127, ext, 0.0).astype(i32))
            j = s % per_row
            moved = pltpu.roll(ext, (j * rays - 64) % 128, 1)
            inside = (lane1 >= j * rays) & (lane1 < (j + 1) * rays)
            row = jnp.where(inside, moved, row)
            if j == per_row - 1:
                data[s // per_row : s // per_row + 1, :] = row
        w[pl.ds(pos, CH), :] = jnp.zeros((CH, 128), f32)
        b[pl.ds(pos, CH), :] = jnp.zeros((CH, 128), f32)
        q[pl.ds(pos, CH), :] = jnp.full((CH, 128), -1.0, f32)
        total[0] = pos
        group_tiles(pos, cell, w, gcell, gw, base, more)
        scatter_tiles(pos, gcell, gw, base, more, b, acc)
        g[0:ROWS_M, :] = acc[:, :DEP]
        g[ROWS_M:COLS, :] = acc[:, DEP:]
        lo[...] = g[: 2 * CLAT, :]
        hi[...] = g[COLS - 2 * CLAT :, :]

    return kernel


def ray_onehots(q):
    qi = q[...].astype(i32)
    lane = iota(qi.shape, 1)
    return jnp.where((qi >> 7) == lane, 1.0, 0.0), (qi & 127) == lane


def forward_kernel(ray_rows):
    def kernel(total, base, more, src, gcell, gw, q, y, gh, gl, got, yv):
        for half in range(2):
            rows = slice(half * ROWS_M, (half + 1) * ROWS_M)
            cols = slice(half * DEP, (half + 1) * DEP)
            high, low = split(src[rows, :])
            gh[:, cols] = high.astype(bf16)
            gl[:, cols] = low.astype(bf16)
        gather_tiles(total[0], gcell, gw, base, more, gh, gl, got, yv)
        oh, ql = ray_onehots(q)
        ys = jnp.where(ql, jnp.sum(yv[...], axis=1, keepdims=True), 0.0)
        full = lax.dot_general(
            oh,
            ys,
            (((0,), (0,)), ((), ())),
            precision=lax.Precision.HIGHEST,
            preferred_element_type=f32,
        )
        y[...] = full[:ray_rows, :]

    return kernel


def send_copies(out, devices, rows):
    count = len(rows)

    def one(d, carry):
        for i, row in enumerate(rows):
            out[d * count + i] = row
        return carry

    lax.fori_loop(0, devices, one, 0)


SIDE = (2, CLON + 2, DEP)


def edge_kernel(devices, ray_rows):
    def kernel(g, before, after, y, la, lb, out):
        for out_ref, lats in ((la, (0, 1)), (lb, (CLAT - 1, CLAT - 2))):
            for k, at in enumerate(lats):
                out_ref[k, 1 : CLON + 1, :] = lat_rows(g, at)
                out_ref[k, 0:1, :] = before[CLAT + at : CLAT + at + 1, :]
                out_ref[k, CLON + 1 : CLON + 2, :] = after[at : at + 1, :]
        gg = jnp.zeros((CLAT, DEP), f32)
        for i in range(CLON):
            c = g[i * CLAT : (i + 1) * CLAT, :]
            gg = gg + c * c
        send_copies(out, devices, [y[i : i + 1, :] for i in range(ray_rows)] + [colsum(gg)])

    return kernel


def received(recv, devices, count):
    def one(d, acc):
        return acc + recv[pl.ds(d * count, count)]

    return lax.fori_loop(0, devices, one, jnp.zeros((count, 1, 128), f32))


def all_rows(acc, start, count):
    return jnp.concatenate([acc[start + i] for i in range(count)], axis=0)


def total_of(x):
    return jnp.sum(jnp.sum(x, axis=0, keepdims=True), axis=1, keepdims=True)


def in_lanes(numbers):
    lane = iota((1, 128), 1)
    packed = jnp.zeros((1, 128), f32)
    for i, x in enumerate(numbers):
        packed = jnp.where(lane == i, x, packed)
    return packed


def second_kernel(devices, ray_rows):
    def kernel(
        total, base, more, place, recv, data_ref, g, before, after, side_before, side_after, gcell, gw, q,
        z, lo, hi, la, lb, q1, p1_ref, r2_ref, num, b, acc, qb, qa, qlb, qla,
    ):
        data = data_ref[...]
        got = received(recv, devices, ray_rows + 1)
        p1 = all_rows(got, 0, ray_rows)
        gg = total_of(got[ray_rows])
        beta1 = jnp.sqrt(total_of(data * data))
        nrm = jnp.sqrt(gg)
        alpha1 = nrm / beta1
        r2 = p1 / nrm - alpha1 * (data / beta1)
        p1_ref[...] = p1
        r2_ref[...] = r2
        num[...] = in_lanes([nrm, beta1, alpha1, total_of(r2 * r2), gg])
        oh, ql = ray_onehots(q)
        padded = jnp.concatenate([r2, jnp.zeros((128 - ray_rows, 128), f32)], axis=0)
        picked = jnp.dot(oh, padded, precision=lax.Precision.HIGHEST, preferred_element_type=f32)
        picked = jnp.sum(jnp.where(ql, picked, 0.0), axis=1, keepdims=True)
        b[...] = jnp.broadcast_to(picked, b.shape)
        scatter_tiles(total[0], gcell, gw, base, more, b, acc)

        near_b = side_before[0, 1 : CLON + 1, :]
        near_a = side_after[0, 1 : CLON + 1, :]
        for out_ref, near, far, side, edge in (
            (qlb, near_b, side_before, 0, 0),
            (qla, near_a, side_after, CLAT - 1, 1),
        ):
            res = depth_part(near) - far[0, 0:CLON, :] - far[0, 2 : CLON + 2, :]
            res = res - far[1, 1 : CLON + 1, :] - lat_rows(g, side)
            out_ref[...] = jnp.where(place[edge] == 0, 0.0, res)
        qb[...] = stencil_rows(
            before[CLAT:, :], before[:CLAT, :], g[:CLAT, :], side_before[0, 0:1, :], side_after[0, 0:1, :]
        )
        qa[...] = stencil_rows(
            after[:CLAT, :], g[COLS - CLAT :, :], after[CLAT:, :],
            side_before[0, CLON + 1 :, :], side_after[0, CLON + 1 :, :],
        )
        for i in range(CLON):
            c = g[i * CLAT : (i + 1) * CLAT, :]
            up = before[CLAT:, :] if i == 0 else g[(i - 1) * CLAT : i * CLAT, :]
            down = after[:CLAT, :] if i == CLON - 1 else g[(i + 1) * CLAT : (i + 2) * CLAT, :]
            q1[i * CLAT : (i + 1) * CLAT, :] = stencil_rows(
                c, up, down, near_b[i : i + 1, :], near_a[i : i + 1, :]
            )
        scale = (damping * damping) / nrm
        for i in range(CLON):
            half, at = divmod(i * CLAT, ROWS_M)
            h = acc[at : at + CLAT, half * DEP : (half + 1) * DEP]
            z[i * CLAT : (i + 1) * CLAT, :] = h + scale * stencil_layer(i, q1, qb, qa, qlb, qla)
        layers(z, lo, hi, la, lb)

    return kernel


def last_smooth_kernel(devices, ray_rows):
    def kernel(z, g, q1, before, after, lat_before, lat_after, y, out):
        sums = [jnp.zeros((CLAT, DEP), f32) for _ in range(5)]
        for i in range(CLON):
            res = stencil_layer(i, z, before, after, lat_before, lat_after)
            rows = slice(i * CLAT, (i + 1) * CLAT)
            c, q, first = z[rows, :], q1[rows, :], g[rows, :]
            terms = [c * c, c * first, res * res, res * q, q * q]
            sums = [x + t for x, t in zip(sums, terms)]
        row = in_lanes([total_of(x) for x in sums])
        send_copies(out, devices, [y[i : i + 1, :] for i in range(ray_rows)] + [row])

    return kernel


def final_kernel(devices, ray_rows, rays):
    def kernel(me, recv, data, p1, r2, num, g, z, model, misfit):
        got = received(recv, devices, ray_rows + 1)
        p2 = all_rows(got, 0, ray_rows)
        nums = got[ray_rows]
        zz, zg, ll, lq, qq = [nums[0:1, i : i + 1] for i in range(5)]
        nrm, beta1, alpha1, rr, gg = [num[0:1, i : i + 1] for i in range(5)]
        beta2 = jnp.sqrt(rr + (damping * damping) * (qq / gg))
        kappa = (beta2 * beta2) / nrm
        size = jnp.sqrt(zz - 2.0 * kappa * zg + kappa * kappa * gg)
        lw = ll - 2.0 * kappa * lq + kappa * kappa * qq
        lwq = lq - kappa * qq
        alpha2 = size / beta2
        av1 = p1[...] / nrm
        av2 = (p2 - kappa * p1[...]) / size
        r3 = av2 - alpha2 * (r2[...] / beta2)
        x = alpha2 / (nrm * beta2)
        grid = (lw / size - 2.0 * x * lwq) / size + (x * x) * qq
        beta3sq = total_of(r3 * r3) + (damping * damping) * grid
        rho = jnp.sqrt(alpha1 * alpha1 + beta2 * beta2)
        cosine = alpha1 / rho
        sine = beta2 / rho
        theta = sine * alpha2
        rho_bar = -cosine * alpha2
        k1 = cosine * beta1 / rho
        t = theta / rho
        phi_bar = sine * beta1
        rho2 = jnp.sqrt(rho_bar * rho_bar + beta3sq)
        k2 = (rho_bar / rho2) * phi_bar / rho2
        first = k1 - k2 * t
        second = k2 / size
        model[...] = (first / nrm - second * kappa) * g[...] + second * z[...]
        mis = data[...] - (first * av1 + k2 * av2)
        per_row = 128 // rays
        d = me[0]
        sub = iota(mis.shape, 0)
        mine = colsum(jnp.where(sub == d // per_row, mis, 0.0))
        misfit[...] = pltpu.roll(mine, (128 - (d % per_row) * rays) % 128, 1)

    return kernel


def exchange_all(x):
    return lax.all_to_all(x, AXES, split_axis=0, concat_axis=0, tiled=True)


def ring(axis, wrap):
    n = lax.axis_size(axis)
    up = [(i, (i + 1) % n) for i in range(n if wrap else n - 1)]
    return up, [(j, i) for i, j in up]


def lon_halo(lo, hi):
    up, down = ring("lon", True)
    return lax.ppermute(hi, "lon", up), lax.ppermute(lo, "lon", down)


def lat_halo(la, lb):
    up, down = ring("lat", False)
    return lax.ppermute(lb, "lat", up), lax.ppermute(la, "lat", down)


def shards(travel_times, ray_counts, tile_brick, cell_offsets, cell_depths, seg_lengths):
    devices = lax.axis_size(AXES)
    rays, per_ray, segs = cell_offsets.shape
    tiles = rays * per_ray
    slots = 2 * tiles
    cap = slots // devices
    width = 2 * cap + 1
    ray_rows = devices * rays // 128
    room = slots + CH
    flat = lambda x: x.reshape(tiles, segs)
    layer_outs = [sds(s) for s in LAYERS]
    grid = sds((COLS, DEP))
    buf = lambda dtype: pltpu.VMEM((ROWS_M, ROWS_N), dtype)

    (packed,) = call(
        pack_kernel(devices, cap, rays, per_ray),
        [sds((devices * width, 1, 128))],
        [SM, SM, SM, VM, VM, VM],
        (tile_brick.T, ray_counts, travel_times, flat(cell_offsets), flat(cell_depths), flat(seg_lengths)),
        [pltpu.VMEM((tiles, segs), f32)] * 2 + [pltpu.SMEM((devices,), i32)],
        name="pack",
    )
    recv0 = exchange_all(packed)
    chunks = room // CH
    grouped = sds((chunks * GROUPS, LANES))
    g, lo, hi, gcell, gw, q, data, total, base, more = call(
        start_kernel(devices, cap, rays),
        [grid, sds((2 * CLAT, DEP)), sds((2 * CLAT, DEP)), grouped, grouped, sds((room, 128)), sds((ray_rows, 128)),
         sds((1,), i32), sds((chunks * GROUPS,), i32), sds((chunks,), i32)],
        [VM],
        (recv0,),
        [pltpu.VMEM((room, 128), f32)] * 3 + [buf(f32)],
        out_specs=[VM] * 7 + [SM] * 3,
        name="start",
    )
    gather_scratch = [buf(bf16), buf(bf16), pltpu.VMEM((1, LANES), f32), pltpu.VMEM((room, 128), f32)]
    tiles_of = (total, base, more)
    before, after = lon_halo(lo, hi)
    (y1,) = call(
        forward_kernel(ray_rows), [sds((ray_rows, 128))], [SM] * 3 + [VM] * 4, (*tiles_of, g, gcell, gw, q),
        gather_scratch, name="forward",
    )
    la, lb, send = call(
        edge_kernel(devices, ray_rows),
        [sds(SIDE), sds(SIDE), sds((devices * (ray_rows + 1), 1, 128))],
        [VM] * 4,
        (g, before, after, y1),
        name="edge",
    )
    sides = lat_halo(la, lb)
    recv1 = exchange_all(send)
    lat = lax.axis_index("lat")
    place = jnp.stack([lat, lax.axis_size("lat") - 1 - lat]).astype(i32)
    z, lo, hi, la, lb, q1, p1, r2, num = call(
        second_kernel(devices, ray_rows),
        [grid, *layer_outs, grid, sds((ray_rows, 128)), sds((ray_rows, 128)), sds((1, 128))],
        [SM] * 4 + [VM] * 10,
        (*tiles_of, place, recv1, data, g, before, after, *sides, gcell, gw, q),
        [pltpu.VMEM((room, 128), f32), buf(f32)] + [pltpu.VMEM((CLAT, DEP), f32)] * 4,
        name="second",
    )
    around = lon_halo(lo, hi) + lat_halo(la, lb)
    (y2,) = call(
        forward_kernel(ray_rows), [sds((ray_rows, 128))], [SM] * 3 + [VM] * 4, (*tiles_of, z, gcell, gw, q),
        gather_scratch, name="forward",
    )
    (send,) = call(
        last_smooth_kernel(devices, ray_rows),
        [sds((devices * (ray_rows + 1), 1, 128))],
        [VM] * 8,
        (z, g, q1, *around, y2),
        name="last_smooth",
    )
    recv2 = exchange_all(send)
    me = lax.axis_index(AXES).astype(i32).reshape(1)
    model, mis = call(
        final_kernel(devices, ray_rows, rays),
        [grid, sds((1, 128))],
        [SM] + [VM] * 7,
        (me, recv2, data, p1, r2, num, g, z),
        name="final",
    )
    return model.reshape(CLON, CLAT, DEP), mis[0, :rays]


def solution(mesh):
    placed = (
        P(("lon", "lat")),
        P(("lon", "lat")),
        P(("lon", "lat"), None),
        P(("lon", "lat"), None, None),
        P(("lon", "lat"), None, None),
        P(("lon", "lat"), None, None),
    )
    return jax.shard_map(
        shards,
        mesh=mesh,
        in_specs=placed,
        out_specs=(P("lon", "lat", None), P(("lon", "lat"))),
        check_vma=False,
    )
```

```python
import jax
import jax.numpy as jnp
from jax import lax
from jax.experimental import pallas as pl
from jax.experimental.pallas import tpu as pltpu
from jax.sharding import PartitionSpec as P

CLON = 32
CLAT = 32
DEP = 128
COLS = CLON * CLAT
ROWS_M = COLS // 2
ROWS_N = 2 * DEP
CH = 16
BLOCK = 16
WIN = 192

damping = 0.01
AXES = ("lon", "lat")
f32 = jnp.float32
i32 = jnp.int32
bf16 = jnp.bfloat16
SM = pl.BlockSpec(memory_space=pltpu.SMEM)
VM = pl.BlockSpec(memory_space=pltpu.VMEM)


def iota(shape, dim):
    return lax.broadcasted_iota(i32, shape, dim)


def sds(shape, dtype=f32):
    return jax.ShapeDtypeStruct(shape, dtype)


def call(kernel, outs, ins, args, scratch=(), out_specs=None, name=None):
    return pl.pallas_call(
        kernel,
        out_shape=outs,
        in_specs=list(ins),
        out_specs=out_specs if out_specs is not None else [VM] * len(outs),
        scratch_shapes=list(scratch),
        name=name,
    )(*args)


def lane_gather(x, index):
    return jnp.take_along_axis(x, index, axis=1, mode="promise_in_bounds")


def lane_order(m):
    lane = iota(m.shape, 1)
    key = m * 128 + lane
    size = 2
    while size <= 128:
        step = size // 2
        while step:
            other = lane_gather(key, lane ^ step)
            keep_low = ((lane & step) == 0) == ((lane & size) == 0)
            key = jnp.where(keep_low, jnp.minimum(key, other), jnp.maximum(key, other))
            step //= 2
        size *= 2
    return key & 127


def pack_kernel(devices, cap, rays, per_ray):
    width = 2 * cap + 1

    def kernel(brick, counts, times, offs, deps, lens, out, cells, lengths, used):
        lane = iota((1, 128), 1)
        out[...] = jnp.zeros_like(out)
        for i in range(0, offs.shape[0], 8):
            at = slice(i, i + 8)
            o = offs[at, :]
            m = o & (ROWS_M - 1)
            order = lane_order(m)
            key = (m * ROWS_N + (o >> 9) * DEP + deps[at, :]).astype(f32)
            cells[at, :] = lane_gather(key, order)
            lengths[at, :] = lane_gather(lens[at, :], order)

        def clear(d, carry):
            used[d] = 0
            return carry

        lax.fori_loop(0, devices, clear, 0)

        def one(r, row):
            value = times[r]
            for j in range(per_ray):
                b = brick[j, r]
                k = used[b]
                used[b] = k + 1
                base = b * width
                out[base + k] = cells[pl.ds(r * per_ray + j, 1), :]
                out[base + cap + k] = lengths[pl.ds(r * per_ray + j, 1), :]
                extra = out[base + 2 * cap]
                extra = jnp.where(lane == k, r.astype(f32), extra)
                out[base + 2 * cap] = jnp.where(lane == 16 + k, value, extra)
            return jnp.where(lane == 64 + r, value, row)

        row = lax.fori_loop(0, counts[0], one, jnp.zeros((1, 128), f32))

        def finish(d, carry):
            at = d * width + 2 * cap
            extra = jnp.where(lane >= 64, row, out[at])
            out[at] = jnp.where(lane == 127, used[d].astype(f32), extra)
            return carry

        lax.fori_loop(0, devices, finish, 0)

    return kernel


def split(x):
    high = x.astype(bf16).astype(f32)
    return high, x - high


def own_block():
    return (iota((8, 128), 1) >> (BLOCK.bit_length() - 1)) == iota((8, 128), 0)


def side_by_side(rows):
    mine = own_block()
    return jnp.concatenate(
        [colsum(jnp.where(mine, rows[8 * h : 8 * h + 8, :], 0.0)) for h in range(CH // 8)], axis=1
    )


GROUPS = 128 // BLOCK
LANES = CH * BLOCK
WINS = [128, 176] + [WIN] * (GROUPS - 4) + [176, 128]


def group_chunk(c, cell, w, gcell, gw, base, more):
    at = pl.multiple_of(c * CH, CH)
    turn = lambda ref: jnp.concatenate(
        [
            pltpu.roll(ref[pl.ds(at + 8 * h, 8), :], 0, 1, stride=BLOCK, stride_axis=0)
            for h in range(CH // 8)
        ],
        axis=0,
    )
    cells = turn(cell)
    lens = turn(w)
    rest = jnp.int32(0)
    for j in range(GROUPS):
        shift = (128 - j * BLOCK) % 128
        gc = side_by_side(pltpu.roll(cells, shift, 1) if j else cells)
        gl = side_by_side(pltpu.roll(lens, shift, 1) if j else lens)
        gcell[pl.ds(c * GROUPS + j, 1), :] = gc
        gw[pl.ds(c * GROUPS + j, 1), :] = gl
        m = gc.astype(i32) >> 8
        low = jnp.min(jnp.where(gl != 0.0, m, ROWS_M - 1))
        high = jnp.max(jnp.where(gl != 0.0, m, 0))
        first = jnp.minimum((low >> 4) << 4, ROWS_M - WINS[j])
        base[c * GROUPS + j] = first
        rest = jnp.maximum(rest, high - first + 1 - WINS[j])
    more[c] = (rest + WIN - 1) // WIN


def main_window(c, j, base, m):
    at = pl.multiple_of(base[c * GROUPS + j], 16)
    return at, m - at, WINS[j]


def more_window(c, i, base, m):
    j = i % GROUPS
    start = base[c * GROUPS + j] + (i // GROUPS) * WIN
    for k, rows in enumerate(WINS):
        start = start + jnp.where(j == k, rows, 0)
    at = pl.multiple_of(jnp.minimum(start, ROWS_M - WIN), 16)
    return at, jnp.where(m >= start, m - at, -1), WIN


def down(row, rows):
    tile = jnp.broadcast_to(row.astype(f32), (16, row.shape[1])).astype(bf16)
    return jnp.concatenate([tile] * (rows // 16), axis=0)


def row_ids(rows):
    return iota((rows, LANES), 0).astype(f32).astype(bf16)


def chunks_of(total):
    return (total + CH - 1) // CH


def scatter_tiles(total, gcell, gw, base, more, b_ref, acc, ahead=None):
    acc[...] = jnp.zeros_like(acc)
    ids = row_ids(ROWS_N)
    one = jnp.ones((), bf16)
    zero = jnp.zeros((), bf16)
    dims = (((1,), (1,)), ((), ()))

    def group(c, j, window, b):
        g = c * GROUPS + j % GROUPS
        ci = gcell[pl.ds(g, 1), :].astype(i32)
        at, m, rows = window(c, j, base, ci >> 8)
        high, low = split(gw[pl.ds(g, 1), :] * b)
        ohm = jnp.where(ids[:rows] == down(m, rows), one, zero)
        hit = ids == down(ci & (ROWS_N - 1), ROWS_N)
        vh = jnp.where(hit, down(high, ROWS_N), zero)
        vl = jnp.where(hit, down(low, ROWS_N), zero)
        acc[pl.ds(at, rows), :] += lax.dot_general(
            ohm, vh, dims, preferred_element_type=f32
        ) + lax.dot_general(ohm, vl, dims, preferred_element_type=f32)

    def chunk(c, carry):
        at = pl.multiple_of(c * CH, CH)
        b = side_by_side(b_ref[pl.ds(at, CH), :])
        for j in range(GROUPS):
            group(c, j, main_window, b)
        if ahead is not None:
            ahead(c + 1)

        @pl.when(more[c] > 0)
        def _():
            def again(i, carry):
                group(c, i, more_window, b)
                return carry

            lax.fori_loop(0, more[c] * GROUPS, again, 0)

        return carry

    if ahead is not None:
        ahead(0)
    lax.fori_loop(0, chunks_of(total), chunk, 0)


def gather_tiles(total, gcell, gw, base, more, gh, gl, got, yv):
    yv[...] = jnp.zeros_like(yv)
    ids = row_ids(ROWS_N)
    one = jnp.ones((), bf16)
    zero = jnp.zeros((), bf16)

    def group(c, j, window):
        g = c * GROUPS + j % GROUPS
        ci = gcell[pl.ds(g, 1), :].astype(i32)
        at, m, rows = window(c, j, base, ci >> 8)
        ohn = jnp.where(ids == down(ci & (ROWS_N - 1), ROWS_N), one, zero)
        full = jnp.dot(gh[pl.ds(at, rows), :], ohn, preferred_element_type=f32) + jnp.dot(
            gl[pl.ds(at, rows), :], ohn, preferred_element_type=f32
        )
        return colsum(jnp.where(iota((rows, LANES), 0) == m, full, 0.0)) * gw[pl.ds(g, 1), :]

    def chunk(c, carry):
        part = group(c, 0, main_window)
        for j in range(1, GROUPS):
            part = part + group(c, j, main_window)
        got[...] = part

        @pl.when(more[c] > 0)
        def _():
            def again(i, carry):
                got[...] += group(c, i, more_window)
                return carry

            lax.fori_loop(0, more[c] * GROUPS, again, 0)

        mine = own_block()
        for h in range(CH // 8):
            at = pl.multiple_of(c * CH + 8 * h, 8)
            yv[pl.ds(at, 8), :] = jnp.where(mine, got[:, 128 * h : 128 * (h + 1)], 0.0)
        return carry

    lax.fori_loop(0, chunks_of(total), chunk, 0)


def lat_rows(src, at):
    return src[pl.ds(at, CLON, stride=CLAT), :]


def layers(src, lo, hi, la, lb):
    lo[...] = src[0:CLAT, :]
    hi[...] = src[COLS - CLAT : COLS, :]
    la[...] = lat_rows(src, 0)
    lb[...] = lat_rows(src, CLAT - 1)


LAYERS = [(CLAT, DEP), (CLAT, DEP), (CLON, DEP), (CLON, DEP)]


def depth_part(c):
    lane = iota(c.shape, 1)
    dm = jnp.where(lane == 0, 0.0, pltpu.roll(c, 1, 1))
    dp = jnp.where(lane == DEP - 1, 0.0, pltpu.roll(c, DEP - 1, 1))
    return 6.0 * c - dm - dp


def stencil_rows(c, up, down, lat_before, lat_after):
    sub = iota(c.shape, 0)
    lm = jnp.where(sub == 0, lat_before, pltpu.roll(c, 1, 0))
    lp = jnp.where(sub == CLAT - 1, lat_after, pltpu.roll(c, CLAT - 1, 0))
    return depth_part(c) - up - down - lm - lp


def stencil_layer(i, src, before, after, lat_before, lat_after):
    c = src[i * CLAT : (i + 1) * CLAT, :]
    up = before[...] if i == 0 else src[(i - 1) * CLAT : i * CLAT, :]
    down = after[...] if i == CLON - 1 else src[(i + 1) * CLAT : (i + 2) * CLAT, :]
    return stencil_rows(c, up, down, lat_before[i : i + 1, :], lat_after[i : i + 1, :])


def colsum(x):
    return jnp.sum(x, axis=0, keepdims=True)


def start_kernel(devices, cap, rays):
    width = 2 * cap + 1

    def kernel(
        recv, g, lo, hi, gcell, gw, q, data, total, base, more, cell, w, b, acc
    ):
        sub = iota((cap, 128), 0)
        lane = iota((cap, 128), 1)
        lane1 = iota((1, 128), 1)
        q[...] = jnp.full_like(q, -1.0)
        per_row = 128 // rays
        pos = 0
        row = jnp.zeros((1, 128), f32)
        for s in range(devices):
            at = s * width
            ext = recv[at + 2 * cap]
            wide = jnp.broadcast_to(ext, (cap, 128))
            qs = jnp.sum(jnp.where(lane == sub, wide, 0.0), axis=1, keepdims=True)
            bs = jnp.sum(jnp.where(lane == sub + 16, wide, 0.0), axis=1, keepdims=True)
            cell[pl.ds(pos, cap), :] = jnp.concatenate([recv[at + k] for k in range(cap)], axis=0)
            w[pl.ds(pos, cap), :] = jnp.concatenate(
                [recv[at + cap + k] for k in range(cap)], axis=0
            )
            q[pl.ds(pos, cap), :] = jnp.broadcast_to(qs + float(s * rays), (cap, 128))
            b[pl.ds(pos, cap), :] = jnp.broadcast_to(bs, (cap, 128))
            pos = pos + jnp.max(jnp.where(lane1 == 127, ext, 0.0).astype(i32))
            j = s % per_row
            moved = pltpu.roll(ext, (j * rays - 64) % 128, 1)
            inside = (lane1 >= j * rays) & (lane1 < (j + 1) * rays)
            row = jnp.where(inside, moved, row)
            if j == per_row - 1:
                data[s // per_row : s // per_row + 1, :] = row
        w[pl.ds(pos, CH), :] = jnp.zeros((CH, 128), f32)
        b[pl.ds(pos, CH), :] = jnp.zeros((CH, 128), f32)
        q[pl.ds(pos, CH), :] = jnp.full((CH, 128), -1.0, f32)
        total[0] = pos
        ahead = lambda c: group_chunk(c, cell, w, gcell, gw, base, more)
        scatter_tiles(pos, gcell, gw, base, more, b, acc, ahead)
        g[0:ROWS_M, :] = acc[:, :DEP]
        g[ROWS_M:COLS, :] = acc[:, DEP:]
        lo[...] = g[: 2 * CLAT, :]
        hi[...] = g[COLS - 2 * CLAT :, :]

    return kernel


def ray_places(q):
    qi = q[...].astype(i32)
    return qi >> 7, (qi & 127) == iota(qi.shape, 1)


def forward_kernel(ray_rows):
    def kernel(total, base, more, src, gcell, gw, q, y, gh, gl, got, yv):
        for half in range(2):
            rows = slice(half * ROWS_M, (half + 1) * ROWS_M)
            cols = slice(half * DEP, (half + 1) * DEP)
            high, low = split(src[rows, :])
            gh[:, cols] = high.astype(bf16)
            gl[:, cols] = low.astype(bf16)
        gather_tiles(total[0], gcell, gw, base, more, gh, gl, got, yv)
        high, here = ray_places(q)
        ys = jnp.where(here, jnp.sum(yv[...], axis=1, keepdims=True), 0.0)
        for i in range(ray_rows):
            y[i : i + 1, :] = colsum(jnp.where(high == i, ys, 0.0))

    return kernel


def send_copies(out, devices, rows):
    count = len(rows)

    def one(d, carry):
        for i, row in enumerate(rows):
            out[d * count + i] = row
        return carry

    lax.fori_loop(0, devices, one, 0)


SIDE = (2, CLON + 2, DEP)


def edge_kernel(devices, ray_rows):
    def kernel(g, before, after, y, la, lb, out):
        for out_ref, lats in ((la, (0, 1)), (lb, (CLAT - 1, CLAT - 2))):
            for k, at in enumerate(lats):
                out_ref[k, 1 : CLON + 1, :] = lat_rows(g, at)
                out_ref[k, 0:1, :] = before[CLAT + at : CLAT + at + 1, :]
                out_ref[k, CLON + 1 : CLON + 2, :] = after[at : at + 1, :]
        gg = jnp.zeros((CLAT, DEP), f32)
        for i in range(CLON):
            c = g[i * CLAT : (i + 1) * CLAT, :]
            gg = gg + c * c
        send_copies(out, devices, [y[i : i + 1, :] for i in range(ray_rows)] + [colsum(gg)])

    return kernel


def received(recv, devices, count):
    def one(d, acc):
        return acc + recv[pl.ds(d * count, count)]

    return lax.fori_loop(0, devices, one, jnp.zeros((count, 1, 128), f32))


def all_rows(acc, start, count):
    return jnp.concatenate([acc[start + i] for i in range(count)], axis=0)


def total_of(x):
    return jnp.sum(jnp.sum(x, axis=0, keepdims=True), axis=1, keepdims=True)


def in_lanes(numbers):
    lane = iota((1, 128), 1)
    packed = jnp.zeros((1, 128), f32)
    for i, x in enumerate(numbers):
        packed = jnp.where(lane == i, x, packed)
    return packed


def second_kernel(devices, ray_rows):
    def kernel(
        total, base, more, place, recv, data_ref, g, before, after, side_before, side_after, gcell, gw, q,
        z, lo, hi, la, lb, q1, p1_ref, r2_ref, num, b, acc, qb, qa, qlb, qla,
    ):
        data = data_ref[...]
        got = received(recv, devices, ray_rows + 1)
        p1 = all_rows(got, 0, ray_rows)
        gg = total_of(got[ray_rows])
        beta1 = jnp.sqrt(total_of(data * data))
        nrm = jnp.sqrt(gg)
        alpha1 = nrm / beta1
        r2 = p1 / nrm - alpha1 * (data / beta1)
        p1_ref[...] = p1
        r2_ref[...] = r2
        num[...] = in_lanes([nrm, beta1, alpha1, total_of(r2 * r2), gg])
        high, here = ray_places(q)
        picked = jnp.zeros(q.shape, f32)
        for i in range(ray_rows):
            picked = jnp.where(high == i, r2[i : i + 1, :], picked)
        picked = jnp.sum(jnp.where(here, picked, 0.0), axis=1, keepdims=True)
        b[...] = jnp.broadcast_to(picked, b.shape)
        scatter_tiles(total[0], gcell, gw, base, more, b, acc)

        near_b = side_before[0, 1 : CLON + 1, :]
        near_a = side_after[0, 1 : CLON + 1, :]
        for out_ref, near, far, side, edge in (
            (qlb, near_b, side_before, 0, 0),
            (qla, near_a, side_after, CLAT - 1, 1),
        ):
            res = depth_part(near) - far[0, 0:CLON, :] - far[0, 2 : CLON + 2, :]
            res = res - far[1, 1 : CLON + 1, :] - lat_rows(g, side)
            out_ref[...] = jnp.where(place[edge] == 0, 0.0, res)
        qb[...] = stencil_rows(
            before[CLAT:, :], before[:CLAT, :], g[:CLAT, :], side_before[0, 0:1, :], side_after[0, 0:1, :]
        )
        qa[...] = stencil_rows(
            after[:CLAT, :], g[COLS - CLAT :, :], after[CLAT:, :],
            side_before[0, CLON + 1 :, :], side_after[0, CLON + 1 :, :],
        )
        for i in range(CLON):
            c = g[i * CLAT : (i + 1) * CLAT, :]
            up = before[CLAT:, :] if i == 0 else g[(i - 1) * CLAT : i * CLAT, :]
            down = after[:CLAT, :] if i == CLON - 1 else g[(i + 1) * CLAT : (i + 2) * CLAT, :]
            q1[i * CLAT : (i + 1) * CLAT, :] = stencil_rows(
                c, up, down, near_b[i : i + 1, :], near_a[i : i + 1, :]
            )
        scale = (damping * damping) / nrm
        for i in range(CLON):
            half, at = divmod(i * CLAT, ROWS_M)
            h = acc[at : at + CLAT, half * DEP : (half + 1) * DEP]
            z[i * CLAT : (i + 1) * CLAT, :] = h + scale * stencil_layer(i, q1, qb, qa, qlb, qla)
        layers(z, lo, hi, la, lb)

    return kernel


def last_smooth_kernel(devices, ray_rows):
    def kernel(z, g, q1, before, after, lat_before, lat_after, y, out):
        sums = [jnp.zeros((CLAT, DEP), f32) for _ in range(5)]
        for i in range(CLON):
            res = stencil_layer(i, z, before, after, lat_before, lat_after)
            rows = slice(i * CLAT, (i + 1) * CLAT)
            c, q, first = z[rows, :], q1[rows, :], g[rows, :]
            terms = [c * c, c * first, res * res, res * q, q * q]
            sums = [x + t for x, t in zip(sums, terms)]
        row = in_lanes([total_of(x) for x in sums])
        send_copies(out, devices, [y[i : i + 1, :] for i in range(ray_rows)] + [row])

    return kernel


def final_kernel(devices, ray_rows, rays):
    def kernel(me, recv, data, p1, r2, num, g, z, model, misfit):
        got = received(recv, devices, ray_rows + 1)
        p2 = all_rows(got, 0, ray_rows)
        nums = got[ray_rows]
        zz, zg, ll, lq, qq = [nums[0:1, i : i + 1] for i in range(5)]
        nrm, beta1, alpha1, rr, gg = [num[0:1, i : i + 1] for i in range(5)]
        beta2 = jnp.sqrt(rr + (damping * damping) * (qq / gg))
        kappa = (beta2 * beta2) / nrm
        size = jnp.sqrt(zz - 2.0 * kappa * zg + kappa * kappa * gg)
        lw = ll - 2.0 * kappa * lq + kappa * kappa * qq
        lwq = lq - kappa * qq
        alpha2 = size / beta2
        av1 = p1[...] / nrm
        av2 = (p2 - kappa * p1[...]) / size
        r3 = av2 - alpha2 * (r2[...] / beta2)
        x = alpha2 / (nrm * beta2)
        grid = (lw / size - 2.0 * x * lwq) / size + (x * x) * qq
        beta3sq = total_of(r3 * r3) + (damping * damping) * grid
        rho = jnp.sqrt(alpha1 * alpha1 + beta2 * beta2)
        cosine = alpha1 / rho
        sine = beta2 / rho
        theta = sine * alpha2
        rho_bar = -cosine * alpha2
        k1 = cosine * beta1 / rho
        t = theta / rho
        phi_bar = sine * beta1
        rho2 = jnp.sqrt(rho_bar * rho_bar + beta3sq)
        k2 = (rho_bar / rho2) * phi_bar / rho2
        first = k1 - k2 * t
        second = k2 / size
        model[...] = (first / nrm - second * kappa) * g[...] + second * z[...]
        mis = data[...] - (first * av1 + k2 * av2)
        per_row = 128 // rays
        d = me[0]
        sub = iota(mis.shape, 0)
        mine = colsum(jnp.where(sub == d // per_row, mis, 0.0))
        misfit[...] = pltpu.roll(mine, (128 - (d % per_row) * rays) % 128, 1)

    return kernel


def exchange_all(x):
    return lax.all_to_all(x, AXES, split_axis=0, concat_axis=0, tiled=True)


def ring(axis, wrap):
    n = lax.axis_size(axis)
    up = [(i, (i + 1) % n) for i in range(n if wrap else n - 1)]
    return up, [(j, i) for i, j in up]


def lon_halo(lo, hi):
    up, down = ring("lon", True)
    return lax.ppermute(hi, "lon", up), lax.ppermute(lo, "lon", down)


def lat_halo(la, lb):
    up, down = ring("lat", False)
    return lax.ppermute(lb, "lat", up), lax.ppermute(la, "lat", down)


def shards(travel_times, ray_counts, tile_brick, cell_offsets, cell_depths, seg_lengths):
    devices = lax.axis_size(AXES)
    rays, per_ray, segs = cell_offsets.shape
    tiles = rays * per_ray
    slots = 2 * tiles
    cap = slots // devices
    width = 2 * cap + 1
    ray_rows = devices * rays // 128
    room = slots + CH
    flat = lambda x: x.reshape(tiles, segs)
    layer_outs = [sds(s) for s in LAYERS]
    grid = sds((COLS, DEP))
    buf = lambda dtype: pltpu.VMEM((ROWS_M, ROWS_N), dtype)

    (packed,) = call(
        pack_kernel(devices, cap, rays, per_ray),
        [sds((devices * width, 1, 128))],
        [SM, SM, SM, VM, VM, VM],
        (tile_brick.T, ray_counts, travel_times, flat(cell_offsets), flat(cell_depths), flat(seg_lengths)),
        [pltpu.VMEM((tiles, segs), f32)] * 2 + [pltpu.SMEM((devices,), i32)],
        name="pack",
    )
    recv0 = exchange_all(packed)
    chunks = room // CH + 1
    grouped = sds((chunks * GROUPS, LANES))
    g, lo, hi, gcell, gw, q, data, total, base, more = call(
        start_kernel(devices, cap, rays),
        [grid, sds((2 * CLAT, DEP)), sds((2 * CLAT, DEP)), grouped, grouped, sds((room, 128)), sds((ray_rows, 128)),
         sds((1,), i32), sds((chunks * GROUPS,), i32), sds((chunks,), i32)],
        [VM],
        (recv0,),
        [pltpu.VMEM((room + CH, 128), f32)] * 2 + [pltpu.VMEM((room, 128), f32), buf(f32)],
        out_specs=[VM] * 7 + [SM] * 3,
        name="start",
    )
    gather_scratch = [buf(bf16), buf(bf16), pltpu.VMEM((1, LANES), f32), pltpu.VMEM((room, 128), f32)]
    tiles_of = (total, base, more)
    before, after = lon_halo(lo, hi)
    (y1,) = call(
        forward_kernel(ray_rows), [sds((ray_rows, 128))], [SM] * 3 + [VM] * 4, (*tiles_of, g, gcell, gw, q),
        gather_scratch, name="forward",
    )
    la, lb, send = call(
        edge_kernel(devices, ray_rows),
        [sds(SIDE), sds(SIDE), sds((devices * (ray_rows + 1), 1, 128))],
        [VM] * 4,
        (g, before, after, y1),
        name="edge",
    )
    sides = lat_halo(la, lb)
    recv1 = exchange_all(send)
    lat = lax.axis_index("lat")
    place = jnp.stack([lat, lax.axis_size("lat") - 1 - lat]).astype(i32)
    z, lo, hi, la, lb, q1, p1, r2, num = call(
        second_kernel(devices, ray_rows),
        [grid, *layer_outs, grid, sds((ray_rows, 128)), sds((ray_rows, 128)), sds((1, 128))],
        [SM] * 4 + [VM] * 10,
        (*tiles_of, place, recv1, data, g, before, after, *sides, gcell, gw, q),
        [pltpu.VMEM((room, 128), f32), buf(f32)] + [pltpu.VMEM((CLAT, DEP), f32)] * 4,
        name="second",
    )
    around = lon_halo(lo, hi) + lat_halo(la, lb)
    (y2,) = call(
        forward_kernel(ray_rows), [sds((ray_rows, 128))], [SM] * 3 + [VM] * 4, (*tiles_of, z, gcell, gw, q),
        gather_scratch, name="forward",
    )
    (send,) = call(
        last_smooth_kernel(devices, ray_rows),
        [sds((devices * (ray_rows + 1), 1, 128))],
        [VM] * 8,
        (z, g, q1, *around, y2),
        name="last_smooth",
    )
    recv2 = exchange_all(send)
    me = lax.axis_index(AXES).astype(i32).reshape(1)
    model, mis = call(
        final_kernel(devices, ray_rows, rays),
        [grid, sds((1, 128))],
        [SM] + [VM] * 7,
        (me, recv2, data, p1, r2, num, g, z),
        name="final",
    )
    return model.reshape(CLON, CLAT, DEP), mis[0, :rays]


def solution(mesh):
    placed = (
        P(("lon", "lat")),
        P(("lon", "lat")),
        P(("lon", "lat"), None),
        P(("lon", "lat"), None, None),
        P(("lon", "lat"), None, None),
        P(("lon", "lat"), None, None),
    )
    return jax.shard_map(
        shards,
        mesh=mesh,
        in_specs=placed,
        out_specs=(P("lon", "lat", None), P(("lon", "lat"))),
        check_vma=False,
    )
```

```python
import jax
import jax.numpy as jnp
from jax import lax
from jax.experimental import pallas as pl
from jax.experimental.pallas import tpu as pltpu
from jax.sharding import PartitionSpec as P

CLON = 32
CLAT = 32
DEP = 128
COLS = CLON * CLAT
ROWS_M = COLS // 2
ROWS_N = 2 * DEP
CH = 16
BLOCK = 16
WIN = 192

damping = 0.01
AXES = ("lon", "lat")
f32 = jnp.float32
i32 = jnp.int32
bf16 = jnp.bfloat16
SM = pl.BlockSpec(memory_space=pltpu.SMEM)
VM = pl.BlockSpec(memory_space=pltpu.VMEM)


def iota(shape, dim):
    return lax.broadcasted_iota(i32, shape, dim)


def sds(shape, dtype=f32):
    return jax.ShapeDtypeStruct(shape, dtype)


def near(shape, dtype=f32):
    return pltpu.VMEM(shape, dtype)


def call(kernel, outs, ins, args, scratch=(), out_specs=None, name=None, keep=True):
    if keep:
        args = [
            pltpu.with_memory_space_constraint(x, pltpu.VMEM) if spec is VM else x
            for x, spec in zip(args, ins)
        ]
    return pl.pallas_call(
        kernel,
        out_shape=outs,
        in_specs=list(ins),
        out_specs=out_specs if out_specs is not None else [VM] * len(outs),
        scratch_shapes=list(scratch),
        compiler_params=pltpu.CompilerParams(vmem_limit_bytes=20 << 20),
        name=name,
    )(*args)


def lane_gather(x, index):
    return jnp.take_along_axis(x, index, axis=1, mode="promise_in_bounds")


def lane_order(m):
    lane = iota(m.shape, 1)
    key = m * 128 + lane
    size = 2
    while size <= 128:
        step = size // 2
        while step:
            other = lane_gather(key, lane ^ step)
            keep_low = ((lane & step) == 0) == ((lane & size) == 0)
            key = jnp.where(keep_low, jnp.minimum(key, other), jnp.maximum(key, other))
            step //= 2
        size *= 2
    return key & 127


def pack_kernel(devices, cap, rays, per_ray):
    width = 2 * cap + 1

    def kernel(brick, counts, times, offs, deps, lens, out, cells, lengths, used):
        lane = iota((1, 128), 1)
        out[...] = jnp.zeros_like(out)
        for i in range(0, offs.shape[0], 8):
            at = slice(i, i + 8)
            o = offs[at, :]
            m = o & (ROWS_M - 1)
            order = lane_order(m)
            key = (m * ROWS_N + (o >> 9) * DEP + deps[at, :]).astype(f32)
            cells[at, :] = lane_gather(key, order)
            lengths[at, :] = lane_gather(lens[at, :], order)

        def clear(d, carry):
            used[d] = 0
            return carry

        lax.fori_loop(0, devices, clear, 0)

        def one(r, row):
            value = times[r]
            for j in range(per_ray):
                b = brick[j, r]
                k = used[b]
                used[b] = k + 1
                base = b * width
                out[base + k] = cells[pl.ds(r * per_ray + j, 1), :]
                out[base + cap + k] = lengths[pl.ds(r * per_ray + j, 1), :]
                extra = out[base + 2 * cap]
                extra = jnp.where(lane == k, r.astype(f32), extra)
                out[base + 2 * cap] = jnp.where(lane == 16 + k, value, extra)
            return jnp.where(lane == 64 + r, value, row)

        row = lax.fori_loop(0, counts[0], one, jnp.zeros((1, 128), f32))

        def finish(d, carry):
            at = d * width + 2 * cap
            extra = jnp.where(lane >= 64, row, out[at])
            out[at] = jnp.where(lane == 127, used[d].astype(f32), extra)
            return carry

        lax.fori_loop(0, devices, finish, 0)

    return kernel


def split(x):
    high = x.astype(bf16).astype(f32)
    return high, x - high


def own_block():
    return (iota((8, 128), 1) >> (BLOCK.bit_length() - 1)) == iota((8, 128), 0)


def side_by_side(rows):
    mine = own_block()
    return jnp.concatenate(
        [colsum(jnp.where(mine, rows[8 * h : 8 * h + 8, :], 0.0)) for h in range(CH // 8)], axis=1
    )


GROUPS = 128 // BLOCK
LANES = CH * BLOCK
WINS = [128, 176] + [WIN] * (GROUPS - 4) + [176, 128]


def group_chunk(c, cell, w, gcell, gw, base, more):
    at = pl.multiple_of(c * CH, CH)
    turn = lambda ref: jnp.concatenate(
        [
            pltpu.roll(ref[pl.ds(at + 8 * h, 8), :], 0, 1, stride=BLOCK, stride_axis=0)
            for h in range(CH // 8)
        ],
        axis=0,
    )
    cells = turn(cell)
    lens = turn(w)
    rest = jnp.int32(0)
    for j in range(GROUPS):
        shift = (128 - j * BLOCK) % 128
        gc = side_by_side(pltpu.roll(cells, shift, 1) if j else cells)
        gl = side_by_side(pltpu.roll(lens, shift, 1) if j else lens)
        gcell[pl.ds(c * GROUPS + j, 1), :] = gc
        gw[pl.ds(c * GROUPS + j, 1), :] = gl
        m = gc.astype(i32) >> 8
        low = jnp.min(jnp.where(gl != 0.0, m, ROWS_M - 1))
        high = jnp.max(jnp.where(gl != 0.0, m, 0))
        first = jnp.minimum((low >> 4) << 4, ROWS_M - WINS[j])
        base[c * GROUPS + j] = first
        rest = jnp.maximum(rest, high - first + 1 - WINS[j])
    more[c] = (rest + WIN - 1) // WIN


def main_window(c, j, base, m):
    at = pl.multiple_of(base[c * GROUPS + j], 16)
    return at, m - at, WINS[j]


def more_window(c, i, base, m):
    j = i % GROUPS
    start = base[c * GROUPS + j] + (i // GROUPS) * WIN
    for k, rows in enumerate(WINS):
        start = start + jnp.where(j == k, rows, 0)
    at = pl.multiple_of(jnp.minimum(start, ROWS_M - WIN), 16)
    return at, jnp.where(m >= start, m - at, -1), WIN


def down(row, rows):
    tile = jnp.broadcast_to(row.astype(f32), (16, row.shape[1])).astype(bf16)
    return jnp.concatenate([tile] * (rows // 16), axis=0)


def row_ids(rows):
    return iota((rows, LANES), 0).astype(f32).astype(bf16)


def chunks_of(total):
    return (total + CH - 1) // CH


def scatter_tiles(total, gcell, gw, base, more, b_ref, acc, ahead=None):
    acc[...] = jnp.zeros_like(acc)
    ids = row_ids(ROWS_N)
    one = jnp.ones((), bf16)
    zero = jnp.zeros((), bf16)
    dims = (((1,), (1,)), ((), ()))

    def group(c, j, window, b):
        g = c * GROUPS + j % GROUPS
        ci = gcell[pl.ds(g, 1), :].astype(i32)
        at, m, rows = window(c, j, base, ci >> 8)
        high, low = split(gw[pl.ds(g, 1), :] * b)
        ohm = jnp.where(ids[:rows] == down(m, rows), one, zero)
        hit = ids == down(ci & (ROWS_N - 1), ROWS_N)
        vh = jnp.where(hit, down(high, ROWS_N), zero)
        vl = jnp.where(hit, down(low, ROWS_N), zero)
        acc[pl.ds(at, rows), :] += lax.dot_general(
            ohm, vh, dims, preferred_element_type=f32
        ) + lax.dot_general(ohm, vl, dims, preferred_element_type=f32)

    def chunk(c, carry):
        at = pl.multiple_of(c * CH, CH)
        b = side_by_side(b_ref[pl.ds(at, CH), :])
        for j in range(GROUPS):
            group(c, j, main_window, b)
        if ahead is not None:
            ahead(c + 1)

        @pl.when(more[c] > 0)
        def _():
            def again(i, carry):
                group(c, i, more_window, b)
                return carry

            lax.fori_loop(0, more[c] * GROUPS, again, 0)

        return carry

    if ahead is not None:
        ahead(0)
    lax.fori_loop(0, chunks_of(total), chunk, 0)


def gather_tiles(total, gcell, gw, base, more, gh, gl, got, yv):
    yv[...] = jnp.zeros_like(yv)
    ids = row_ids(ROWS_N)
    one = jnp.ones((), bf16)
    zero = jnp.zeros((), bf16)

    def group(c, j, window):
        g = c * GROUPS + j % GROUPS
        ci = gcell[pl.ds(g, 1), :].astype(i32)
        at, m, rows = window(c, j, base, ci >> 8)
        ohn = jnp.where(ids == down(ci & (ROWS_N - 1), ROWS_N), one, zero)
        full = jnp.dot(gh[pl.ds(at, rows), :], ohn, preferred_element_type=f32) + jnp.dot(
            gl[pl.ds(at, rows), :], ohn, preferred_element_type=f32
        )
        return colsum(jnp.where(iota((rows, LANES), 0) == m, full, 0.0)) * gw[pl.ds(g, 1), :]

    def chunk(c, carry):
        part = group(c, 0, main_window)
        for j in range(1, GROUPS):
            part = part + group(c, j, main_window)
        got[...] = part

        @pl.when(more[c] > 0)
        def _():
            def again(i, carry):
                got[...] += group(c, i, more_window)
                return carry

            lax.fori_loop(0, more[c] * GROUPS, again, 0)

        mine = own_block()
        for h in range(CH // 8):
            at = pl.multiple_of(c * CH + 8 * h, 8)
            yv[pl.ds(at, 8), :] = jnp.where(mine, got[:, 128 * h : 128 * (h + 1)], 0.0)
        return carry

    lax.fori_loop(0, chunks_of(total), chunk, 0)


def lat_rows(src, at):
    return src[pl.ds(at, CLON, stride=CLAT), :]


def layers(src, lo, hi, la, lb):
    lo[...] = src[0:CLAT, :]
    hi[...] = src[COLS - CLAT : COLS, :]
    la[...] = lat_rows(src, 0)
    lb[...] = lat_rows(src, CLAT - 1)


LAYERS = [(CLAT, DEP), (CLAT, DEP), (CLON, DEP), (CLON, DEP)]


def depth_part(c):
    lane = iota(c.shape, 1)
    dm = jnp.where(lane == 0, 0.0, pltpu.roll(c, 1, 1))
    dp = jnp.where(lane == DEP - 1, 0.0, pltpu.roll(c, DEP - 1, 1))
    return 6.0 * c - dm - dp


def stencil_rows(c, up, down, lat_before, lat_after):
    sub = iota(c.shape, 0)
    lm = jnp.where(sub == 0, lat_before, pltpu.roll(c, 1, 0))
    lp = jnp.where(sub == CLAT - 1, lat_after, pltpu.roll(c, CLAT - 1, 0))
    return depth_part(c) - up - down - lm - lp


def stencil_layer(i, src, before, after, lat_before, lat_after):
    c = src[i * CLAT : (i + 1) * CLAT, :]
    up = before[...] if i == 0 else src[(i - 1) * CLAT : i * CLAT, :]
    down = after[...] if i == CLON - 1 else src[(i + 1) * CLAT : (i + 2) * CLAT, :]
    return stencil_rows(c, up, down, lat_before[i : i + 1, :], lat_after[i : i + 1, :])


def colsum(x):
    return jnp.sum(x, axis=0, keepdims=True)


def start_kernel(devices, cap, rays):
    width = 2 * cap + 1

    def kernel(
        recv, g, lo, hi, gcell, gw, q, data, total, base, more, cell, w, b, acc
    ):
        sub = iota((cap, 128), 0)
        lane = iota((cap, 128), 1)
        lane1 = iota((1, 128), 1)
        q[...] = jnp.full_like(q, -1.0)
        per_row = 128 // rays
        pos = 0
        row = jnp.zeros((1, 128), f32)
        for s in range(devices):
            at = s * width
            ext = recv[at + 2 * cap]
            wide = jnp.broadcast_to(ext, (cap, 128))
            qs = jnp.sum(jnp.where(lane == sub, wide, 0.0), axis=1, keepdims=True)
            bs = jnp.sum(jnp.where(lane == sub + 16, wide, 0.0), axis=1, keepdims=True)
            cell[pl.ds(pos, cap), :] = jnp.concatenate([recv[at + k] for k in range(cap)], axis=0)
            w[pl.ds(pos, cap), :] = jnp.concatenate(
                [recv[at + cap + k] for k in range(cap)], axis=0
            )
            q[pl.ds(pos, cap), :] = jnp.broadcast_to(qs + float(s * rays), (cap, 128))
            b[pl.ds(pos, cap), :] = jnp.broadcast_to(bs, (cap, 128))
            pos = pos + jnp.max(jnp.where(lane1 == 127, ext, 0.0).astype(i32))
            j = s % per_row
            moved = pltpu.roll(ext, (j * rays - 64) % 128, 1)
            inside = (lane1 >= j * rays) & (lane1 < (j + 1) * rays)
            row = jnp.where(inside, moved, row)
            if j == per_row - 1:
                data[s // per_row : s // per_row + 1, :] = row
        w[pl.ds(pos, CH), :] = jnp.zeros((CH, 128), f32)
        b[pl.ds(pos, CH), :] = jnp.zeros((CH, 128), f32)
        q[pl.ds(pos, CH), :] = jnp.full((CH, 128), -1.0, f32)
        total[0] = pos
        ahead = lambda c: group_chunk(c, cell, w, gcell, gw, base, more)
        scatter_tiles(pos, gcell, gw, base, more, b, acc, ahead)
        g[0:ROWS_M, :] = acc[:, :DEP]
        g[ROWS_M:COLS, :] = acc[:, DEP:]
        lo[...] = g[: 2 * CLAT, :]
        hi[...] = g[COLS - 2 * CLAT :, :]

    return kernel


def ray_places(q):
    qi = q[...].astype(i32)
    return qi >> 7, (qi & 127) == iota(qi.shape, 1)


def forward_kernel(ray_rows):
    def kernel(total, base, more, src, gcell, gw, q, y, gh, gl, got, yv):
        for half in range(2):
            rows = slice(half * ROWS_M, (half + 1) * ROWS_M)
            cols = slice(half * DEP, (half + 1) * DEP)
            high, low = split(src[rows, :])
            gh[:, cols] = high.astype(bf16)
            gl[:, cols] = low.astype(bf16)
        gather_tiles(total[0], gcell, gw, base, more, gh, gl, got, yv)
        high, here = ray_places(q)
        ys = jnp.where(here, jnp.sum(yv[...], axis=1, keepdims=True), 0.0)
        for i in range(ray_rows):
            y[i : i + 1, :] = colsum(jnp.where(high == i, ys, 0.0))

    return kernel


def send_copies(out, devices, rows):
    count = len(rows)

    def one(d, carry):
        for i, row in enumerate(rows):
            out[d * count + i] = row
        return carry

    lax.fori_loop(0, devices, one, 0)


SIDE = (2, CLON + 2, DEP)


def edge_kernel(devices, ray_rows):
    def kernel(g, before, after, y, la, lb, out):
        for out_ref, lats in ((la, (0, 1)), (lb, (CLAT - 1, CLAT - 2))):
            for k, at in enumerate(lats):
                out_ref[k, 1 : CLON + 1, :] = lat_rows(g, at)
                out_ref[k, 0:1, :] = before[CLAT + at : CLAT + at + 1, :]
                out_ref[k, CLON + 1 : CLON + 2, :] = after[at : at + 1, :]
        gg = jnp.zeros((CLAT, DEP), f32)
        for i in range(CLON):
            c = g[i * CLAT : (i + 1) * CLAT, :]
            gg = gg + c * c
        send_copies(out, devices, [y[i : i + 1, :] for i in range(ray_rows)] + [colsum(gg)])

    return kernel


def received(recv, devices, count):
    def one(d, acc):
        return acc + recv[pl.ds(d * count, count)]

    return lax.fori_loop(0, devices, one, jnp.zeros((count, 1, 128), f32))


def all_rows(acc, start, count):
    return jnp.concatenate([acc[start + i] for i in range(count)], axis=0)


def total_of(x):
    return jnp.sum(jnp.sum(x, axis=0, keepdims=True), axis=1, keepdims=True)


def in_lanes(numbers):
    lane = iota((1, 128), 1)
    packed = jnp.zeros((1, 128), f32)
    for i, x in enumerate(numbers):
        packed = jnp.where(lane == i, x, packed)
    return packed


def second_kernel(devices, ray_rows):
    def kernel(
        total, base, more, place, recv, data_ref, g, before, after, side_before, side_after, gcell, gw, q,
        z, lo, hi, la, lb, q1, p1_ref, r2_ref, num, b, acc, qb, qa, qlb, qla,
    ):
        data = data_ref[...]
        got = received(recv, devices, ray_rows + 1)
        p1 = all_rows(got, 0, ray_rows)
        gg = total_of(got[ray_rows])
        beta1 = jnp.sqrt(total_of(data * data))
        nrm = jnp.sqrt(gg)
        alpha1 = nrm / beta1
        r2 = p1 / nrm - alpha1 * (data / beta1)
        p1_ref[...] = p1
        r2_ref[...] = r2
        num[...] = in_lanes([nrm, beta1, alpha1, total_of(r2 * r2), gg])
        high, here = ray_places(q)
        picked = jnp.zeros(q.shape, f32)
        for i in range(ray_rows):
            picked = jnp.where(high == i, r2[i : i + 1, :], picked)
        picked = jnp.sum(jnp.where(here, picked, 0.0), axis=1, keepdims=True)
        b[...] = jnp.broadcast_to(picked, b.shape)
        scatter_tiles(total[0], gcell, gw, base, more, b, acc)

        near_b = side_before[0, 1 : CLON + 1, :]
        near_a = side_after[0, 1 : CLON + 1, :]
        for out_ref, near, far, side, edge in (
            (qlb, near_b, side_before, 0, 0),
            (qla, near_a, side_after, CLAT - 1, 1),
        ):
            res = depth_part(near) - far[0, 0:CLON, :] - far[0, 2 : CLON + 2, :]
            res = res - far[1, 1 : CLON + 1, :] - lat_rows(g, side)
            out_ref[...] = jnp.where(place[edge] == 0, 0.0, res)
        qb[...] = stencil_rows(
            before[CLAT:, :], before[:CLAT, :], g[:CLAT, :], side_before[0, 0:1, :], side_after[0, 0:1, :]
        )
        qa[...] = stencil_rows(
            after[:CLAT, :], g[COLS - CLAT :, :], after[CLAT:, :],
            side_before[0, CLON + 1 :, :], side_after[0, CLON + 1 :, :],
        )
        for i in range(CLON):
            c = g[i * CLAT : (i + 1) * CLAT, :]
            up = before[CLAT:, :] if i == 0 else g[(i - 1) * CLAT : i * CLAT, :]
            down = after[:CLAT, :] if i == CLON - 1 else g[(i + 1) * CLAT : (i + 2) * CLAT, :]
            q1[i * CLAT : (i + 1) * CLAT, :] = stencil_rows(
                c, up, down, near_b[i : i + 1, :], near_a[i : i + 1, :]
            )
        scale = (damping * damping) / nrm
        for i in range(CLON):
            half, at = divmod(i * CLAT, ROWS_M)
            h = acc[at : at + CLAT, half * DEP : (half + 1) * DEP]
            z[i * CLAT : (i + 1) * CLAT, :] = h + scale * stencil_layer(i, q1, qb, qa, qlb, qla)
        layers(z, lo, hi, la, lb)

    return kernel


def last_smooth_kernel(devices, ray_rows):
    def kernel(z, g, q1, before, after, lat_before, lat_after, y, out):
        sums = [jnp.zeros((CLAT, DEP), f32) for _ in range(5)]
        for i in range(CLON):
            res = stencil_layer(i, z, before, after, lat_before, lat_after)
            rows = slice(i * CLAT, (i + 1) * CLAT)
            c, q, first = z[rows, :], q1[rows, :], g[rows, :]
            terms = [c * c, c * first, res * res, res * q, q * q]
            sums = [x + t for x, t in zip(sums, terms)]
        row = in_lanes([total_of(x) for x in sums])
        send_copies(out, devices, [y[i : i + 1, :] for i in range(ray_rows)] + [row])

    return kernel


def final_kernel(devices, ray_rows, rays):
    def kernel(me, recv, data, p1, r2, num, g, z, model, misfit):
        got = received(recv, devices, ray_rows + 1)
        p2 = all_rows(got, 0, ray_rows)
        nums = got[ray_rows]
        zz, zg, ll, lq, qq = [nums[0:1, i : i + 1] for i in range(5)]
        nrm, beta1, alpha1, rr, gg = [num[0:1, i : i + 1] for i in range(5)]
        beta2 = jnp.sqrt(rr + (damping * damping) * (qq / gg))
        kappa = (beta2 * beta2) / nrm
        size = jnp.sqrt(zz - 2.0 * kappa * zg + kappa * kappa * gg)
        lw = ll - 2.0 * kappa * lq + kappa * kappa * qq
        lwq = lq - kappa * qq
        alpha2 = size / beta2
        av1 = p1[...] / nrm
        av2 = (p2 - kappa * p1[...]) / size
        r3 = av2 - alpha2 * (r2[...] / beta2)
        x = alpha2 / (nrm * beta2)
        grid = (lw / size - 2.0 * x * lwq) / size + (x * x) * qq
        beta3sq = total_of(r3 * r3) + (damping * damping) * grid
        rho = jnp.sqrt(alpha1 * alpha1 + beta2 * beta2)
        cosine = alpha1 / rho
        sine = beta2 / rho
        theta = sine * alpha2
        rho_bar = -cosine * alpha2
        k1 = cosine * beta1 / rho
        t = theta / rho
        phi_bar = sine * beta1
        rho2 = jnp.sqrt(rho_bar * rho_bar + beta3sq)
        k2 = (rho_bar / rho2) * phi_bar / rho2
        first = k1 - k2 * t
        second = k2 / size
        model[...] = (first / nrm - second * kappa) * g[...] + second * z[...]
        mis = data[...] - (first * av1 + k2 * av2)
        per_row = 128 // rays
        d = me[0]
        sub = iota(mis.shape, 0)
        mine = colsum(jnp.where(sub == d // per_row, mis, 0.0))
        misfit[...] = pltpu.roll(mine, (128 - (d % per_row) * rays) % 128, 1)

    return kernel


def exchange_all(x):
    return lax.all_to_all(x, AXES, split_axis=0, concat_axis=0, tiled=True)


def ring(axis, wrap):
    n = lax.axis_size(axis)
    up = [(i, (i + 1) % n) for i in range(n if wrap else n - 1)]
    return up, [(j, i) for i, j in up]


def lon_halo(lo, hi):
    up, down = ring("lon", True)
    return lax.ppermute(hi, "lon", up), lax.ppermute(lo, "lon", down)


def lat_halo(la, lb):
    up, down = ring("lat", False)
    return lax.ppermute(lb, "lat", up), lax.ppermute(la, "lat", down)


def shards(travel_times, ray_counts, tile_brick, cell_offsets, cell_depths, seg_lengths):
    devices = lax.axis_size(AXES)
    rays, per_ray, segs = cell_offsets.shape
    tiles = rays * per_ray
    slots = 2 * tiles
    cap = slots // devices
    width = 2 * cap + 1
    ray_rows = devices * rays // 128
    room = slots + CH
    flat = lambda x: x.reshape(tiles, segs)
    layer_outs = [near(s) for s in LAYERS]
    grid = near((COLS, DEP))
    buf = lambda dtype: pltpu.VMEM((ROWS_M, ROWS_N), dtype)

    (packed,) = call(
        pack_kernel(devices, cap, rays, per_ray),
        [near((devices * width, 1, 128))],
        [SM, SM, SM, VM, VM, VM],
        (tile_brick.T, ray_counts, travel_times, flat(cell_offsets), flat(cell_depths), flat(seg_lengths)),
        [pltpu.VMEM((tiles, segs), f32)] * 2 + [pltpu.SMEM((devices,), i32)],
        name="pack",
        keep=False,
    )
    recv0 = exchange_all(packed)
    chunks = room // CH + 1
    grouped = near((chunks * GROUPS, LANES))
    g, lo, hi, gcell, gw, q, data, total, base, more = call(
        start_kernel(devices, cap, rays),
        [grid, near((2 * CLAT, DEP)), near((2 * CLAT, DEP)), grouped, grouped, near((room, 128)), near((ray_rows, 128)),
         sds((1,), i32), sds((chunks * GROUPS,), i32), sds((chunks,), i32)],
        [VM],
        (recv0,),
        [pltpu.VMEM((room + CH, 128), f32)] * 2 + [pltpu.VMEM((room, 128), f32), buf(f32)],
        out_specs=[VM] * 7 + [SM] * 3,
        name="start",
    )
    gather_scratch = [buf(bf16), buf(bf16), pltpu.VMEM((1, LANES), f32), pltpu.VMEM((room, 128), f32)]
    tiles_of = (total, base, more)
    before, after = lon_halo(lo, hi)
    (y1,) = call(
        forward_kernel(ray_rows), [near((ray_rows, 128))], [SM] * 3 + [VM] * 4, (*tiles_of, g, gcell, gw, q),
        gather_scratch, name="forward",
    )
    la, lb, send = call(
        edge_kernel(devices, ray_rows),
        [near(SIDE), near(SIDE), near((devices * (ray_rows + 1), 1, 128))],
        [VM] * 4,
        (g, before, after, y1),
        name="edge",
    )
    sides = lat_halo(la, lb)
    recv1 = exchange_all(send)
    lat = lax.axis_index("lat")
    place = jnp.stack([lat, lax.axis_size("lat") - 1 - lat]).astype(i32)
    z, lo, hi, la, lb, q1, p1, r2, num = call(
        second_kernel(devices, ray_rows),
        [grid, *layer_outs, grid, near((ray_rows, 128)), near((ray_rows, 128)), near((1, 128))],
        [SM] * 4 + [VM] * 10,
        (*tiles_of, place, recv1, data, g, before, after, *sides, gcell, gw, q),
        [pltpu.VMEM((room, 128), f32), buf(f32)] + [pltpu.VMEM((CLAT, DEP), f32)] * 4,
        name="second",
    )
    around = lon_halo(lo, hi) + lat_halo(la, lb)
    (y2,) = call(
        forward_kernel(ray_rows), [near((ray_rows, 128))], [SM] * 3 + [VM] * 4, (*tiles_of, z, gcell, gw, q),
        gather_scratch, name="forward",
    )
    (send,) = call(
        last_smooth_kernel(devices, ray_rows),
        [near((devices * (ray_rows + 1), 1, 128))],
        [VM] * 8,
        (z, g, q1, *around, y2),
        name="last_smooth",
    )
    recv2 = exchange_all(send)
    me = lax.axis_index(AXES).astype(i32).reshape(1)
    model, mis = call(
        final_kernel(devices, ray_rows, rays),
        [sds((COLS, DEP)), sds((1, 128))],
        [SM] + [VM] * 7,
        (me, recv2, data, p1, r2, num, g, z),
        name="final",
    )
    return model.reshape(CLON, CLAT, DEP), mis[0, :rays]


def solution(mesh):
    placed = (
        P(("lon", "lat")),
        P(("lon", "lat")),
        P(("lon", "lat"), None),
        P(("lon", "lat"), None, None),
        P(("lon", "lat"), None, None),
        P(("lon", "lat"), None, None),
    )
    return jax.shard_map(
        shards,
        mesh=mesh,
        in_specs=placed,
        out_specs=(P("lon", "lat", None), P(("lon", "lat"))),
        check_vma=False,
    )
```
